32 devices in a mesh: grp: 4 (over y, x), slab: 8 (over z, core).
Axes of the slice: x: 2, y: 2, z: 4, core: 2. Of those that a mesh axis runs over, the one named last changes fastest.
Arguments:
- state: float32 [4, 2, 256, 128, 256], P(None, None, 'grp', 'slab'), may hold values from -5.6 to 5.6
- kz_group: int32 [256], replicated, may hold values from 0 to 7, as said below
- cutoffs: int32 [3], replicated, may hold values from 28 to 32
- damping: float32 [8], replicated, may hold values from 0.005 to 0.5
- power: float32 [8], replicated, may hold values from 0.2 to 4
Outputs:
- new_state: float32 [4, 2, 256, 128, 256], P(None, None, 'grp', 'slab')
The draws below stay inside these ranges and needn't reach their ends.
Inputs may be any that keep to these rules, and one draw needn't show every extreme that they name: `kz_group`: each of the 8 groups holds exactly 32 indices.
All inputs are finite; a program needn't handle non-finite values.
Results may differ from the reference program's by a relative error of at most 0.00005.
Values sent between devices are 32-bit elements; how exact they have to be, the bound alone decides.
A program may use at most 192 MiB of HBM per device.

```python
import math
import jax
import jax.numpy as jnp
from jax import lax

NX = 256
NY = 256
NZ = 256
GROUPS = 8
KX = 128
GMODES = 32


def draw_state(key, part):
    noise = jnp.clip(jax.random.normal(key, (4, 2, NZ, KX, NY), jnp.float32), -4.0, 4.0)
    rate = 0.7
    mixing = 0.6
    decay = jnp.exp(-rate * jnp.arange(KX, dtype=jnp.float32) / KX)[None, None, None, :, None]
    noise = noise * decay
    buoyant = mixing * noise[2] + 0.8 * noise[3]
    return jnp.concatenate([noise[:3], buoyant[None]], axis=0)


def draw_kz_group(key, part):
    ordering = jax.random.permutation(key, NZ)
    return (ordering // (NZ // GROUPS)).astype(jnp.int32)


def setup_inputs(seed: int = 0) -> dict:
    seeds = jax.random.split(jax.random.key(seed), 6)
    return {
        "state": draw_state(jax.random.fold_in(seeds[5], 71), 0),
        "kz_group": draw_kz_group(jax.random.fold_in(seeds[5], 71), 0),
        "cutoffs": jax.random.randint(seeds[2], (3,), 28, 33).astype(jnp.int32),
        "damping": jnp.clip(jnp.exp(jax.random.uniform(seeds[3], (GROUPS,), jnp.float32, math.log(0.005), math.log(0.5))), 0.005, 0.5),
        "power": jnp.clip(jnp.exp(jax.random.uniform(seeds[4], (GROUPS,), jnp.float32, math.log(0.2), math.log(4.0))), 0.2, 4.0),
    }


TIME_STEP = 0.25
CORIOLIS = 1.0
BRUNT_SQUARED = 2.0
EPSILON = 1e-06

def signed(index, length):
    return jnp.where(index < length // 2, index, index - length)

def to_grid(field, slot_mode, weights):
    padded = jnp.zeros((NZ, NX, NY), field.dtype)
    padded = padded.at[slot_mode, :KX, :].set(field * weights[None, :, None])
    return jnp.real(jnp.fft.ifftn(padded)) * math.sqrt(NX * NY * NZ)

def to_spectral(values, slot_mode):
    full = jnp.fft.fftn(values) / math.sqrt(NX * NY * NZ)
    return full[slot_mode][:, :KX, :]

def squared(entries):
    return jnp.real(entries) ** 2 + jnp.imag(entries) ** 2

def reference(state, kz_group, cutoffs, damping, power):
    float_type = state.dtype
    slot_mode = jnp.argsort(kz_group, stable=True).astype(jnp.int32)
    mode_z = signed(slot_mode, NZ)
    mode_x = jnp.arange(KX, dtype=jnp.int32)
    mode_y = signed(jnp.arange(NY, dtype=jnp.int32), NY)
    wave_z = (2.0 * math.pi / NZ * mode_z.astype(float_type))[:, None, None]
    wave_x = (2.0 * math.pi / NX * mode_x.astype(float_type))[None, :, None]
    wave_y = (2.0 * math.pi / NY * mode_y.astype(float_type))[None, None, :]
    spectra = state[:, 0] + 1j * state[:, 1]
    flow_x, flow_y, flow_z, buoyant = (spectra[0], spectra[1], spectra[2], spectra[3])
    swirl_x = 1j * (wave_y * flow_z - wave_z * flow_y)
    swirl_y = 1j * (wave_z * flow_x - wave_x * flow_z)
    swirl_z = 1j * (wave_x * flow_y - wave_y * flow_x)
    weights = jnp.where(mode_x == 0, 1.0, 2.0).astype(float_type)
    grids = [to_grid(field, slot_mode, weights) for field in (flow_x, flow_y, flow_z, buoyant, swirl_x, swirl_y, swirl_z)]
    grid_u, grid_v, grid_w, grid_b, grid_ox, grid_oy, grid_oz = grids
    products = [grid_v * grid_oz - grid_w * grid_oy, grid_w * grid_ox - grid_u * grid_oz, grid_u * grid_oy - grid_v * grid_ox, grid_u * grid_b, grid_v * grid_b, grid_w * grid_b]
    hats = [to_spectral(product, slot_mode) for product in products]
    kept = ((96 * jnp.abs(mode_z) <= cutoffs[2] * NZ)[:, None, None] & (96 * mode_x <= cutoffs[0] * NX)[None, :, None] & (96 * jnp.abs(mode_y) <= cutoffs[1] * NY)[None, None, :]).astype(float_type)
    moment_x, moment_y, moment_z = (kept * hats[0], kept * hats[1], kept * hats[2])
    source_b = -1j * kept * (wave_x * hats[3] + wave_y * hats[4] + wave_z * hats[5])
    cell_flux = jnp.real(flow_z) * jnp.real(buoyant) + jnp.imag(flow_z) * jnp.imag(buoyant)
    cell_energy = 0.5 * (squared(flow_x) + squared(flow_y) + squared(flow_z) + squared(buoyant) / BRUNT_SQUARED)
    modes_total = GMODES * KX * NY
    flux_mean = lax.optimization_barrier(jnp.sum(cell_flux.reshape(GROUPS, -1), axis=1)) / modes_total
    energy_mean = lax.optimization_barrier(jnp.sum(cell_energy.reshape(GROUPS, -1), axis=1)) / modes_total
    forcing = (power - flux_mean) / (2.0 * (energy_mean + EPSILON))
    forcing_slot = jnp.repeat(forcing, GMODES)[:, None, None]
    damping_slot = jnp.repeat(damping, GMODES)[:, None, None]
    right_x = flow_x + TIME_STEP * (moment_x + forcing_slot * flow_x)
    right_y = flow_y + TIME_STEP * (moment_y + forcing_slot * flow_y)
    right_z = flow_z + TIME_STEP * (moment_z + forcing_slot * flow_z)
    right_b = buoyant + TIME_STEP * source_b
    wave_sq = wave_x * wave_x + wave_y * wave_y + wave_z * wave_z
    implicit = 1.0 + TIME_STEP * damping_slot * wave_sq
    rotation = TIME_STEP * CORIOLIS
    first_den = implicit * implicit + rotation * rotation
    second_den = implicit * implicit + TIME_STEP * TIME_STEP * BRUNT_SQUARED
    new_x = (implicit * right_x + rotation * right_y) / first_den
    new_y = (implicit * right_y - rotation * right_x) / first_den
    new_z = (implicit * right_z + TIME_STEP * right_b) / second_den
    new_b = (implicit * right_b - TIME_STEP * BRUNT_SQUARED * right_z) / second_den
    inverse_sq = 1.0 / (wave_sq + (wave_sq == 0).astype(float_type))
    inner = (wave_x * new_x + wave_y * new_y + wave_z * new_z) * inverse_sq
    new_x = new_x - wave_x * inner
    new_y = new_y - wave_y * inner
    new_z = new_z - wave_z * inner
    return jnp.stack([jnp.stack([jnp.real(updated), jnp.imag(updated)]) for updated in (new_x, new_y, new_z, new_b)]).astype(float_type)
```

```python
import functools
import math

import jax
import jax.numpy as jnp
import numpy as np
from jax import lax
from jax.experimental import pallas as pl
from jax.experimental.pallas import tpu as pltpu
from jax.sharding import PartitionSpec as P

TWO_PI = 6.283185307179586
TIME_STEP = 0.25
CORIOLIS = 1.0
BRUNT_SQUARED = 2.0
EPSILON = 1e-06
CHUNKS = 2
FIELDS = 6
RETURNS = 5


def signed(index, length):
    return jnp.where(index < length // 2, index, index - length)


def halves(values):
    high = values.astype(jnp.bfloat16)
    low = (values - high.astype(jnp.float32)).astype(jnp.bfloat16)
    return high, low


def constant_halves(table):
    table = np.asarray(table, np.float32)
    high = table.astype(jnp.bfloat16)
    low = (table - high.astype(np.float32)).astype(jnp.bfloat16)
    return jnp.asarray(high), jnp.asarray(low)


def dot3(left, right, dims=(((1,), (0,)), ((), ()))):
    dot = functools.partial(lax.dot_general, dimension_numbers=dims, preferred_element_type=jnp.float32)
    return dot(left[0], right[0]) + (dot(left[0], right[1]) + dot(left[1], right[0]))


def trig(modes, points, length):
    phase = np.asarray(modes)[:, None] * np.asarray(points)[None, :] % length
    theta = phase * (2.0 * math.pi / length)
    return np.cos(theta), np.sin(theta)


def flat_rows(ref):
    shape = ref.shape
    return ref.reshape(math.prod(shape[:-1]), shape[-1])


def strided(ref, start, count, stride):
    return ref[pl.ds(start, count, stride=stride), :]


def forward_y(cols, slots, width, *refs):
    high_ref, low_ref, out_ref = refs[width:]
    out = flat_rows(out_ref)
    lanes = 2 * slots
    count = high_ref.shape[1] // 2
    rows = [flat_rows(ref) for ref in refs[:width]]
    table = (high_ref[0], low_ref[0])
    sign = jnp.where(lax.broadcasted_iota(jnp.int32, (1, lanes), 1) < slots, -1.0, 1.0)
    pair = 2 if cols % 2 == 0 else 1
    def some(first):
        taken = []
        for j in range(pair):
            for d in range(2):
                start = d * slots * cols + first + j
                taken.append(jnp.concatenate([strided(part, start, slots, cols) for part in rows], axis=1))
        data = halves(jnp.concatenate(taken, axis=0))
        both = dot3(table, data, (((1,), (1,)), ((), ())))
        for j in range(pair):
            part = both[:, j * lanes : (j + 1) * lanes]
            result = part[:count] + sign * pltpu.roll(part[count:], slots, 1)
            out[pl.ds(first + j, count, stride=cols), :] = result

    unrolled = 2 if cols % (2 * pair) == 0 else 1

    def several(i, carry):
        for k in range(unrolled):
            some((i * unrolled + k) * pair)
        return carry

    lax.fori_loop(0, cols // (pair * unrolled), several, 0)


def planes(groups, slabs, x_step, in_ref, zf_refs, xf_refs, xb_refs, zb_refs, kz_ref, out_ref):
    cols, lanes = in_ref.shape[3:]
    kx = slabs * cols
    nz = zf_refs[0].shape[1] // 2

    def field(f):
        parts = []
        for g in range(groups):
            part = in_ref[g * slabs : (g + 1) * slabs, 0, f]
            parts.append(part.reshape(kx, lanes))
        return jnp.concatenate(parts, axis=1)

    u, u_y, w, w_y, v, b = (field(f) for f in range(FIELDS))
    wave_z = kz_ref[0:1, :]
    wave_x = x_step * lax.broadcasted_iota(jnp.int32, (kx, 1), 0).astype(jnp.float32)
    omega_x = w_y - wave_z * v
    omega_y = wave_z * u - wave_x * w
    omega_z = wave_x * v - u_y
    stacked = halves(jnp.concatenate([u, v, w, b, omega_x, omega_y, omega_z], axis=0))
    lines = dot3(stacked, (zf_refs[0][...], zf_refs[1][...]))
    grids = []
    for f in range(7):
        line = lines[f * kx : (f + 1) * kx]
        line = halves(jnp.concatenate([line[:, :nz], line[:, nz:]], axis=0))
        kind = 0 if f < 4 else 1
        grids.append(dot3((xf_refs[0][kind], xf_refs[1][kind]), line))
    gu, gv, gw, gb, gox, goy, goz = grids
    products = [gv * goz - gw * goy, gw * gox - gu * goz, gu * goy - gv * gox, gu * gb, gv * gb, gw * gb]
    table = (xb_refs[0][...], xb_refs[1][...])
    backs = []
    for product in products:
        back = dot3(table, halves(product))
        backs.append(jnp.concatenate([back[:kx], back[kx:]], axis=1))
    spectra = dot3(halves(jnp.concatenate(backs, axis=0)), (zb_refs[0][...], zb_refs[1][...]))
    hats = [spectra[f * kx : (f + 1) * kx] for f in range(6)]
    moved = wave_x * hats[3] + wave_z * hats[5]
    for f, hat in enumerate([hats[0], hats[1], hats[2], moved, hats[4]]):
        for g in range(groups):
            part = hat[:, g * lanes : (g + 1) * lanes]
            out_ref[g * slabs : (g + 1) * slabs, 0, f] = part.reshape(slabs, cols, lanes)


def finish(slots, chunks, width, *refs):
    in_refs = refs[:chunks]
    state_refs = refs[chunks : chunks + width]
    high_ref, low_ref, zrow_ref, xrow_ref, yrow_ref, out_ref = refs[chunks + width : chunks + width + 6]
    out_parts = refs[chunks + width + 6 :]
    block = out_ref.shape[3]
    ny = out_ref.shape[4]
    inputs = [flat_rows(ref) for ref in in_refs]
    state = [flat_rows(ref) for ref in state_refs]
    table = (high_ref[...], low_ref[...])
    wave_z, kept_z, forcing, damping = (zrow_ref[k] for k in range(4))
    wave_y, kept_y = yrow_ref[0:1, :], yrow_ref[1:2, :]

    def load(c, d, x):
        start = (c * 2 + d) * slots * block + x
        return jnp.concatenate([strided(part, start, slots, block) for part in state], axis=1)

    def store(c, d, x, value):
        start = (c * 2 + d) * slots * block + x
        for k in range(width):
            out_parts[k][pl.ds(start, slots, stride=block), :] = value[:, 128 * k : 128 * (k + 1)]

    def one(x, carry):
        columns = []
        for f in range(RETURNS):
            pieces = []
            for rows in inputs:
                count = rows.shape[0] // (RETURNS * block)
                pieces.append(rows[pl.ds(f * block + x, count, stride=RETURNS * block), :])
            columns.append(jnp.concatenate(pieces, axis=0).T)
        both = dot3(halves(jnp.concatenate(columns, axis=0)), table)
        tends = []
        for f in range(RETURNS):
            re = both[2 * f * slots : (2 * f + 1) * slots]
            im = both[(2 * f + 1) * slots : (2 * f + 2) * slots]
            tends.append((re[:, :ny] + im[:, ny:], im[:, :ny] - re[:, ny:]))
        wave_x = xrow_ref[0, pl.ds(x, 1), :]
        kept = (kept_z * kept_y) * xrow_ref[1, pl.ds(x, 1), :]
        kept = kept * TIME_STEP
        wave_sq = wave_x * wave_x + wave_y * wave_y + wave_z * wave_z
        implicit = 1.0 + TIME_STEP * damping * wave_sq
        rotation = TIME_STEP * CORIOLIS
        first = 1.0 / (implicit * implicit + rotation * rotation)
        second = 1.0 / (implicit * implicit + TIME_STEP * TIME_STEP * BRUNT_SQUARED)
        inverse_sq = 1.0 / (wave_sq + (wave_sq == 0).astype(jnp.float32))
        growth = 1.0 + TIME_STEP * forcing
        total = [tends[3][d] + wave_y * tends[4][d] for d in range(2)]
        source = [total[1], -total[0]]
        for d in range(2):
            right_x = growth * load(0, d, x) + kept * tends[0][d]
            right_y = growth * load(1, d, x) + kept * tends[1][d]
            right_z = growth * load(2, d, x) + kept * tends[2][d]
            right_b = load(3, d, x) + kept * source[d]
            new_x = (implicit * right_x + rotation * right_y) * first
            new_y = (implicit * right_y - rotation * right_x) * first
            new_z = (implicit * right_z + TIME_STEP * right_b) * second
            new_b = (implicit * right_b - TIME_STEP * BRUNT_SQUARED * right_z) * second
            inner = (wave_x * new_x + wave_y * new_y + wave_z * new_z) * inverse_sq
            store(0, d, x, new_x - wave_x * inner)
            store(1, d, x, new_y - wave_y * inner)
            store(2, d, x, new_z - wave_z * inner)
            store(3, d, x, new_b)
        return carry

    lax.fori_loop(0, block, one, 0)
    for k in range(width):
        for c in range(4):
            for d in range(2):
                size = slots * block
                part = out_parts[k][(c * 2 + d) * size : (c * 2 + d + 1) * size, :]
                out_ref[c, d, :, :, 128 * k : 128 * (k + 1)] = part.reshape(slots, block, 128)


def whole(array):
    return pl.BlockSpec(array.shape, lambda *_: (0,) * array.ndim)


def shards(state, kz_group, cutoffs, damping, power):
    groups = lax.axis_size("grp")
    slabs = lax.axis_size("slab")
    grp_index = lax.axis_index("grp")
    slab_index = lax.axis_index("slab")
    slots = state.shape[2]
    cols = state.shape[3]
    NY = state.shape[4]
    NZ = slots * groups
    KX = cols * slabs
    NX = 2 * KX
    GROUPS = damping.shape[0]
    GMODES = NZ // GROUPS
    devices = groups * slabs
    rows_here = NY // devices
    groups_here = GROUPS // groups
    chunks = CHUNKS if rows_here % CHUNKS == 0 else 1
    rows_chunk = rows_here // chunks
    lanes = 2 * slots
    width = NY // 128
    normalizer = 1.0 / math.sqrt(NX * NY * NZ)

    mode_y = np.fft.fftfreq(NY, 1.0 / NY).astype(np.int64)
    order_y = np.arange(NY).reshape(devices, chunks, rows_chunk).transpose(1, 0, 2).reshape(-1)
    cos_y, sin_y = trig(order_y, np.arange(NY), NY)
    wave_np = TWO_PI / NY * mode_y
    plain = np.stack([cos_y.reshape(chunks, -1, NY), sin_y.reshape(chunks, -1, NY)], axis=1)
    plain = plain.reshape(chunks, 1, -1, NY)
    y_forward = constant_halves(np.concatenate([plain, plain * wave_np], axis=1))
    y_back = constant_halves(np.concatenate([cos_y, sin_y], axis=1))
    cos_x, sin_x = trig(np.arange(NX), np.arange(KX), NX)
    weights = np.where(np.arange(KX) == 0, 1.0, 2.0)[None, :] * normalizer
    x_forward = constant_halves(
        np.stack(
            [
                np.concatenate([cos_x * weights, -sin_x * weights], axis=1),
                np.concatenate([-sin_x * weights, -cos_x * weights], axis=1),
            ]
        )
    )
    x_back = constant_halves(np.concatenate([cos_x.T, -sin_x.T], axis=0) * normalizer)

    params = pltpu.CompilerParams(vmem_limit_bytes=60 * 1024 * 1024)
    sent_shape = jax.ShapeDtypeStruct((devices, rows_chunk, FIELDS, cols, lanes), jnp.float32)
    flops = 2 * 3 * FIELDS * 2 * NY * NY * cols * lanes // chunks
    sent = []
    for c in range(chunks):
        step = pl.pallas_call(
            functools.partial(forward_y, cols, slots, width),
            grid=(FIELDS,),
            in_specs=[
                pl.BlockSpec(
                    (1, 2, slots, cols, 128),
                    lambda i, k=k: (jnp.where(i < 4, i // 2 * 2, (i - 4) * 2 + 1), 0, 0, 0, k),
                )
                for k in range(width)
            ]
            + [pl.BlockSpec((1, 2 * NY // chunks, NY), lambda i: (jnp.where(i < 4, i % 2, 0), 0, 0))] * 2,
            out_specs=pl.BlockSpec((devices, rows_chunk, 1, cols, lanes), lambda i: (0, 0, i, 0, 0)),
            out_shape=sent_shape,
            compiler_params=params,
            cost_estimate=pl.CostEstimate(flops=flops, bytes_accessed=20 << 20, transcendentals=0),
        )(*[state] * width, y_forward[0][c], y_forward[1][c])
        sent.append(step)

    slot_mode = jnp.argsort(kz_group, stable=True).astype(jnp.int32)
    phase = slot_mode[:, None] * jnp.arange(NZ, dtype=jnp.int32)[None, :] % NZ
    theta = phase.astype(jnp.float32) * (TWO_PI / NZ)
    cos_z = jnp.cos(theta).reshape(groups, 1, slots, NZ)
    sin_z = jnp.sin(theta).reshape(groups, 1, slots, NZ)
    z_real = jnp.concatenate([cos_z, -sin_z], axis=1).reshape(2 * NZ, NZ)
    z_imag = jnp.concatenate([sin_z, cos_z], axis=1).reshape(2 * NZ, NZ)
    z_table = jnp.concatenate([z_real, z_imag], axis=1)
    z_high = lax.reduce_precision(z_table, 8, 7)
    z_low = (z_table - z_high).astype(jnp.bfloat16)
    z_high = z_high.astype(jnp.bfloat16)
    z_forward = (z_high, z_low)
    z_back = (z_high.T, z_low.T)
    wave_all = TWO_PI / NZ * signed(slot_mode, NZ).astype(jnp.float32)
    wave_lanes = jnp.broadcast_to(wave_all.reshape(groups, 1, slots), (groups, 2, slots)).reshape(1, 2 * NZ)
    wave_lanes = jnp.broadcast_to(wave_lanes, (8, 2 * NZ))

    def middle(zf0, zf1, xf0, xf1, xb0, xb1, zb0, zb1, in_ref, kz_ref, out_ref):
        planes(
            groups, slabs, TWO_PI / NX, in_ref, (zf0, zf1), (xf0, xf1), (xb0, xb1), (zb0, zb1), kz_ref, out_ref
        )

    tables = [*z_forward, *x_forward, *x_back, *z_back]
    back_shape = (devices, rows_chunk, RETURNS, cols, lanes)
    flops = 2 * 3 * rows_chunk * NZ * KX * (4 * 13 * NZ + 2 * 13 * NX)
    come = []
    for c in range(chunks):
        got = lax.all_to_all(sent[c], ("grp", "slab"), 0, 0, tiled=True)
        come.append(got)
    left = []
    for c in range(chunks):
        back = pl.pallas_call(
            middle,
            grid=(rows_chunk,),
            in_specs=[whole(t) for t in tables]
            + [pl.BlockSpec((devices, 1, FIELDS, cols, lanes), lambda y: (0, y, 0, 0, 0)), whole(wave_lanes)],
            out_specs=pl.BlockSpec((devices, 1, RETURNS, cols, lanes), lambda y: (0, y, 0, 0, 0)),
            out_shape=jax.ShapeDtypeStruct(back_shape, jnp.float32),
            compiler_params=params,
            cost_estimate=pl.CostEstimate(flops=flops, bytes_accessed=22 << 20, transcendentals=0),
        )(*tables, come[c], wave_lanes)
        left.append(lax.all_to_all(back, ("grp", "slab"), 0, 0, tiled=True))

    real_part = state[:, 0]
    imag_part = state[:, 1]
    cell_flux = real_part[2] * real_part[3] + imag_part[2] * imag_part[3]
    cell_energy = 0.5 * (
        jnp.sum(real_part[:3] ** 2 + imag_part[:3] ** 2, axis=0)
        + (real_part[3] ** 2 + imag_part[3] ** 2) / BRUNT_SQUARED
    )
    partial_value = jnp.stack(
        [jnp.sum(cell_flux, axis=(1, 2)), jnp.sum(cell_energy, axis=(1, 2))], axis=1
    )
    partial_value = jnp.sum(partial_value.reshape(groups_here, GMODES, 2), axis=1)
    means = lax.psum(partial_value, "slab") / (GMODES * KX * NY)
    power_here = lax.dynamic_slice_in_dim(power, grp_index * groups_here, groups_here)
    damping_here = lax.dynamic_slice_in_dim(damping, grp_index * groups_here, groups_here)
    forcing = (power_here - means[:, 0]) / (2.0 * (means[:, 1] + EPSILON))

    local_mode = signed(lax.dynamic_slice_in_dim(slot_mode, grp_index * slots, slots), NZ)
    mode_x = slab_index * cols + jnp.arange(cols, dtype=jnp.int32)
    mode_y = signed(jnp.arange(NY, dtype=jnp.int32), NY)
    zrow = jnp.stack(
        [
            TWO_PI / NZ * local_mode.astype(jnp.float32),
            (96 * jnp.abs(local_mode) <= cutoffs[2] * NZ).astype(jnp.float32),
            jnp.repeat(forcing, GMODES),
            jnp.repeat(damping_here, GMODES),
        ]
    )
    zrow = jnp.broadcast_to(zrow[:, :, None], (4, slots, NY))
    xrow = jnp.stack(
        [
            TWO_PI / NX * mode_x.astype(jnp.float32),
            (96 * mode_x <= cutoffs[0] * NX).astype(jnp.float32),
        ]
    )
    xrow = jnp.broadcast_to(xrow[:, :, None], (2, cols, NY))
    yrow = jnp.stack(
        [
            TWO_PI / NY * mode_y.astype(jnp.float32),
            (96 * jnp.abs(mode_y) <= cutoffs[1] * NY).astype(jnp.float32),
        ]
    )
    block = 8 if cols % 8 == 0 else cols
    return pl.pallas_call(
        functools.partial(finish, slots, chunks, width),
        grid=(cols // block,),
        in_specs=[
            pl.BlockSpec((devices, rows_chunk, RETURNS, block, lanes), lambda i: (0, 0, 0, i, 0))
            for _ in range(chunks)
        ]
        + [pl.BlockSpec((4, 2, slots, block, 128), lambda i, k=k: (0, 0, 0, i, k)) for k in range(width)]
        + [
            whole(y_back[0]),
            whole(y_back[1]),
            whole(zrow),
            pl.BlockSpec((2, block, NY), lambda i: (0, i, 0)),
            whole(yrow),
        ],
        out_specs=pl.BlockSpec((4, 2, slots, block, NY), lambda i: (0, 0, 0, i, 0)),
        out_shape=jax.ShapeDtypeStruct(state.shape, jnp.float32),
        scratch_shapes=[pltpu.VMEM((8 * slots * block, 128), jnp.float32)] * width,
        compiler_params=params,
        cost_estimate=pl.CostEstimate(flops=1 << 33, bytes_accessed=28 << 20, transcendentals=0),
    )(*left, *[state] * width, *y_back, zrow, xrow, yrow)


def solution(mesh):
    return jax.shard_map(
        shards,
        mesh=mesh,
        in_specs=(P(None, None, "grp", "slab", None), P(), P(), P(), P()),
        out_specs=P(None, None, "grp", "slab", None),
        check_vma=False,
    )
```

```python
import functools
import math

import jax
import jax.numpy as jnp
import numpy as np
from jax import lax
from jax.experimental import pallas as pl
from jax.experimental.pallas import tpu as pltpu
from jax.sharding import PartitionSpec as P

TWO_PI = 6.283185307179586
TIME_STEP = 0.25
CORIOLIS = 1.0
BRUNT_SQUARED = 2.0
EPSILON = 1e-06
AHEAD = 3
LAG = 3
WIDEST = 32
FIELDS = 6
RETURNS = 5


def signed(index, length):
    return jnp.where(index < length // 2, index, index - length)


def halves(values):
    high = values.astype(jnp.bfloat16)
    low = (values - high.astype(jnp.float32)).astype(jnp.bfloat16)
    return high, low


def constant_halves(table):
    table = np.asarray(table, np.float32)
    high = table.astype(jnp.bfloat16)
    low = (table - high.astype(np.float32)).astype(jnp.bfloat16)
    return jnp.asarray(high), jnp.asarray(low)


def dot3(left, right, dims=(((1,), (0,)), ((), ()))):
    dot = functools.partial(lax.dot_general, dimension_numbers=dims, preferred_element_type=jnp.float32)
    return dot(left[0], right[0]) + (dot(left[0], right[1]) + dot(left[1], right[0]))


def trig(modes, points, length):
    phase = np.asarray(modes)[:, None] * np.asarray(points)[None, :] % length
    theta = phase * (2.0 * math.pi / length)
    return np.cos(theta), np.sin(theta)


def flat_rows(ref):
    shape = ref.shape
    return ref.reshape(math.prod(shape[:-1]), shape[-1])


def strided(ref, start, count, stride):
    return ref[pl.ds(start, count, stride=stride), :]


def forward_y(cols, slots, width, members, *refs):
    flow_w = [flat_rows(ref) for ref in refs[width : 2 * width]]
    high_ref, low_ref, out_ref, sums_ref = refs[2 * width :]
    out = flat_rows(out_ref)
    lanes = 2 * slots
    count = high_ref.shape[1] // 2
    rows = [flat_rows(ref) for ref in refs[:width]]
    table = (high_ref[0], low_ref[0])
    sign = jnp.where(lax.broadcasted_iota(jnp.int32, (1, lanes), 1) < slots, -1.0, 1.0)
    pair = 2 if cols % 2 == 0 else 1
    def some(first):
        taken = []
        for j in range(pair):
            for d in range(2):
                start = d * slots * cols + first + j
                taken.append(jnp.concatenate([strided(part, start, slots, cols) for part in rows], axis=1))
        data = halves(jnp.concatenate(taken, axis=0))
        both = dot3(table, data, (((1,), (1,)), ((), ())))
        for j in range(pair):
            part = both[:, j * lanes : (j + 1) * lanes]
            result = part[:count] + sign * pltpu.roll(part[count:], slots, 1)
            out[pl.ds(first + j, count, stride=cols), :] = result

    unrolled = 2 if cols % (2 * pair) == 0 else 1

    def several(i, carry):
        for k in range(unrolled):
            some((i * unrolled + k) * pair)
        return carry

    lax.fori_loop(0, cols // (pair * unrolled), several, 0)

    step = pl.program_id(0)
    here = sums_ref.shape[0] // 2
    size = members * cols

    @pl.when(step == 0)
    def _():
        sums_ref[...] = jnp.zeros_like(sums_ref)

    def add_up(which, one, two, weight):
        for group in range(here):
            for d in range(2):
                start = (d * slots + group * members) * cols
                for a, b in zip(one, two):
                    product = a[pl.ds(start, size), :] * b[pl.ds(start, size), :]
                    total = jnp.sum(product.reshape(size // 8, 8, 128), axis=0)
                    sums_ref[which * here + group] += weight * total

    @pl.when((step == 0) | (step == 2) | (step == 4))
    def _():
        add_up(1, rows, rows, 0.5)

    @pl.when(step == 5)
    def _():
        add_up(1, rows, rows, 0.5 / BRUNT_SQUARED)
        add_up(0, rows, flow_w, 1.0)


def planes(groups, slabs, x_step, read, zf_refs, xf_refs, xb_refs, zb_refs, kz_ref, kept_ref, write):
    wave_z = kz_ref[0:1, :]
    nz = zf_refs[0].shape[1] // 2
    u, u_y, w, w_y, v, b = (jnp.concatenate([read(g, f) for g in range(groups)], axis=1) for f in range(FIELDS))
    kx = u.shape[0]
    wave_x = x_step * lax.broadcasted_iota(jnp.int32, (kx, 1), 0).astype(jnp.float32)
    omega_x = w_y - wave_z * v
    omega_y = wave_z * u - wave_x * w
    omega_z = wave_x * v - u_y
    stacked = halves(jnp.concatenate([u, v, w, b, omega_x, omega_y, omega_z], axis=0))
    lines = dot3(stacked, (zf_refs[0][...], zf_refs[1][...]))
    grids = []
    for f in range(7):
        line = lines[f * kx : (f + 1) * kx]
        line = halves(jnp.concatenate([line[:, :nz], line[:, nz:]], axis=0))
        kind = 0 if f < 4 else 1
        grids.append(dot3((xf_refs[0][kind], xf_refs[1][kind]), line))
    gu, gv, gw, gb, gox, goy, goz = grids
    products = [gv * goz - gw * goy, gw * gox - gu * goz, gu * goy - gv * gox, gu * gb, gv * gb, gw * gb]
    table = (xb_refs[0][...], xb_refs[1][...])
    backs = []
    for product in products:
        back = dot3(table, halves(product))
        backs.append(jnp.concatenate([back[:kx], back[kx:]], axis=1))
    spectra = dot3(halves(jnp.concatenate(backs, axis=0)), (zb_refs[0][...], zb_refs[1][...]))
    hats = [spectra[f * kx : (f + 1) * kx] for f in range(6)]
    moved = wave_x * hats[3] + kept_ref[0:1, :] * hats[5]
    for f, hat in enumerate([hats[0], hats[1], hats[2], moved, hats[4]]):
        write(f, hat)


def travel(groups, slabs, x_step, *refs):
    (sent, zf0, zf1, xf0, xf1, xb0, xb1, zb0, zb1, choose, kz_ref, kept_ref, sums_ref, final, totals) = refs[:15]
    (taken, made, kept, ready, f_send, f_recv, f_own, b_send, b_recv, c_send, c_recv, c_own, t_send, t_recv, t_own) = refs[15:]
    devices = groups * slabs
    count = taken.shape[0]
    cols, lanes = taken.shape[3:]
    ahead = min(AHEAD, count)
    lag = min(LAG, count)
    g = lax.axis_index("grp")
    s = lax.axis_index("slab")
    me = g * slabs + s

    def remote(source, target, send, recv, to_g, to_s):
        pltpu.make_async_remote_copy(
            src_ref=source,
            dst_ref=target,
            send_sem=send,
            recv_sem=recv,
            device_id={"grp": to_g, "slab": to_s},
            device_id_type=pl.DeviceIdType.MESH,
        ).start()

    def wait_all(ref, sem):
        pltpu.make_async_copy(ref, ref, sem).wait()

    def own_f(y):
        return pltpu.make_async_copy(sent.at[me, y], taken.at[y, me], f_own.at[y])

    def send_f(y):
        own_f(y).start()

        def one(k, carry):
            to = lax.rem(me + k, devices)
            remote(sent.at[to, y], taken.at[y, me], f_send.at[y], f_recv.at[y], to // slabs, lax.rem(to, slabs))
            return carry

        lax.fori_loop(1, devices, one, 0)

    def send_b(y):
        def one(k, carry):
            to = lax.rem(s + k, slabs)
            remote(made.at[y, to], kept.at[y, s], b_send.at[y], b_recv.at[y], g, to)
            return carry

        lax.fori_loop(1, slabs, one, 0)

    def own_c(y):
        return pltpu.make_async_copy(ready.at[y, g], final.at[g, y], c_own.at[y])

    def send_c(y):
        own_c(y).start()
        for k in range(1, groups):
            to = lax.rem(g + k, groups)
            remote(ready.at[y, to], final.at[g, y], c_send.at[y], c_recv.at[y], to, s)

    own_t = pltpu.make_async_copy(sums_ref, totals.at[s], t_own)

    def first(y, carry):
        send_f(y)
        return carry

    lax.fori_loop(0, ahead, first, 0)
    own_t.start()

    def send_t(k, carry):
        remote(sums_ref, totals.at[s], t_send, t_recv, g, lax.rem(s + k, slabs))
        return carry

    lax.fori_loop(1, slabs, send_t, 0)

    def step(t, carry):
        @pl.when(t < count)
        def _():
            own_f(t).wait()
            wait_all(taken.at[t, pl.ds(0, devices - 1)], f_recv.at[t])

            @pl.when(t + ahead < count)
            def _():
                send_f(t + ahead)

            def read(group, f):
                part = taken[t, group * slabs : (group + 1) * slabs, f]
                return part.reshape(slabs * cols, lanes)

            def write(f, value):
                made[t, :, f] = value.reshape(slabs, cols, value.shape[1])

            planes(
                groups, slabs, x_step, read, (zf0, zf1), (xf0, xf1), (xb0, xb1), (zb0, zb1), kz_ref, kept_ref, write
            )
            kept[t, s] = made[t, s]

        @pl.when(t >= lag)
        def _():
            y = t - lag
            wait_all(kept.at[y, pl.ds(0, slabs - 1)], b_recv.at[y])
            data = kept[y]
            high, low = halves(data.reshape(slabs * RETURNS * cols, data.shape[-1]))
            dot = functools.partial(jnp.dot, preferred_element_type=jnp.float32)
            picked = dot(high, choose[...]) + dot(low, choose[...])
            for group in range(groups):
                part = picked[:, group * lanes : (group + 1) * lanes]
                ready[y, group] = part.reshape(slabs, RETURNS, cols, lanes)

        @pl.when(t < count)
        def _():
            send_b(t)

        @pl.when(t >= lag)
        def _():
            send_c(t - lag)

        return carry

    lax.fori_loop(0, count + lag, step, 0)

    def last(y, carry):
        own_c(y).wait()
        wait_all(final.at[pl.ds(0, groups - 1), y], c_recv.at[y])
        wait_all(taken.at[y, pl.ds(0, devices - 1)], f_send.at[y])
        wait_all(kept.at[y, pl.ds(0, slabs - 1)], b_send.at[y])
        wait_all(ready.at[y, pl.ds(0, groups - 1)], c_send.at[y])
        return carry

    lax.fori_loop(0, count, last, 0)
    own_t.wait()
    wait_all(totals.at[pl.ds(0, slabs - 1)], t_recv)
    wait_all(totals.at[pl.ds(0, slabs - 1)], t_send)


def finish(slots, chunks, width, *refs):
    in_refs = refs[:chunks]
    state_refs = refs[chunks : chunks + width]
    high_ref, low_ref, zrow_ref, xrow_ref, yrow_ref, out_ref = refs[chunks + width : chunks + width + 6]
    out_parts = refs[chunks + width + 6 :]
    block = out_ref.shape[3]
    ny = out_ref.shape[4]
    inputs = [flat_rows(ref) for ref in in_refs]
    state = [flat_rows(ref) for ref in state_refs]
    table = (high_ref[...], low_ref[...])
    wave_z, kept_z, forcing, damping = (zrow_ref[k] for k in range(4))
    wave_y, kept_y = yrow_ref[0:1, :], yrow_ref[1:2, :]

    def load(c, d, x):
        start = (c * 2 + d) * slots * block + x
        return jnp.concatenate([strided(part, start, slots, block) for part in state], axis=1)

    def store(c, d, x, value):
        start = (c * 2 + d) * slots * block + x
        for k in range(width):
            out_parts[k][pl.ds(start, slots, stride=block), :] = value[:, 128 * k : 128 * (k + 1)]

    def one(x, carry):
        columns = []
        for f in range(RETURNS):
            pieces = []
            for rows in inputs:
                count = rows.shape[0] // (RETURNS * block)
                pieces.append(rows[pl.ds(f * block + x, count, stride=RETURNS * block), :])
            columns.append(jnp.concatenate(pieces, axis=0).T)
        both = dot3(halves(jnp.concatenate(columns, axis=0)), table)
        tends = []
        for f in range(RETURNS):
            re = both[2 * f * slots : (2 * f + 1) * slots]
            im = both[(2 * f + 1) * slots : (2 * f + 2) * slots]
            tends.append((re[:, :ny] + im[:, ny:], im[:, :ny] - re[:, ny:]))
        wave_x = xrow_ref[0, pl.ds(x, 1), :]
        kept = (kept_z * kept_y) * xrow_ref[1, pl.ds(x, 1), :]
        kept = kept * TIME_STEP
        wave_sq = wave_x * wave_x + wave_y * wave_y + wave_z * wave_z
        implicit = 1.0 + TIME_STEP * damping * wave_sq
        rotation = TIME_STEP * CORIOLIS
        first = 1.0 / (implicit * implicit + rotation * rotation)
        second = 1.0 / (implicit * implicit + TIME_STEP * TIME_STEP * BRUNT_SQUARED)
        inverse_sq = 1.0 / (wave_sq + (wave_sq == 0).astype(jnp.float32))
        growth = 1.0 + TIME_STEP * forcing
        total = [tends[3][d] + wave_y * tends[4][d] for d in range(2)]
        source = [total[1], -total[0]]
        for d in range(2):
            right_x = growth * load(0, d, x) + kept * tends[0][d]
            right_y = growth * load(1, d, x) + kept * tends[1][d]
            right_z = growth * load(2, d, x) + kept * tends[2][d]
            right_b = load(3, d, x) + kept * source[d]
            new_x = (implicit * right_x + rotation * right_y) * first
            new_y = (implicit * right_y - rotation * right_x) * first
            new_z = (implicit * right_z + TIME_STEP * right_b) * second
            new_b = (implicit * right_b - TIME_STEP * BRUNT_SQUARED * right_z) * second
            inner = (wave_x * new_x + wave_y * new_y + wave_z * new_z) * inverse_sq
            store(0, d, x, new_x - wave_x * inner)
            store(1, d, x, new_y - wave_y * inner)
            store(2, d, x, new_z - wave_z * inner)
            store(3, d, x, new_b)
        return carry

    lax.fori_loop(0, block, one, 0)
    for k in range(width):
        for c in range(4):
            for d in range(2):
                size = slots * block
                part = out_parts[k][(c * 2 + d) * size : (c * 2 + d + 1) * size, :]
                out_ref[c, d, :, :, 128 * k : 128 * (k + 1)] = part.reshape(slots, block, 128)


def whole(array):
    return pl.BlockSpec(array.shape, lambda *_: (0,) * array.ndim)


def shards(state, kz_group, cutoffs, damping, power):
    groups = lax.axis_size("grp")
    slabs = lax.axis_size("slab")
    grp_index = lax.axis_index("grp")
    slab_index = lax.axis_index("slab")
    slots = state.shape[2]
    cols = state.shape[3]
    NY = state.shape[4]
    NZ = slots * groups
    KX = cols * slabs
    NX = 2 * KX
    GROUPS = damping.shape[0]
    GMODES = NZ // GROUPS
    devices = groups * slabs
    rows_here = NY // devices
    groups_here = GROUPS // groups
    lanes = 2 * slots
    width = NY // 128
    normalizer = 1.0 / math.sqrt(NX * NY * NZ)

    mode_y = np.fft.fftfreq(NY, 1.0 / NY).astype(np.int64)
    cos_y, sin_y = trig(np.arange(NY), np.arange(NY), NY)
    wave_np = TWO_PI / NY * mode_y
    plain = np.concatenate([cos_y, sin_y], axis=0)
    y_forward = constant_halves(np.stack([plain, plain * wave_np]))
    order = np.arange(NY).reshape(groups, slabs, rows_here).transpose(0, 2, 1).reshape(-1)
    y_back = constant_halves(np.concatenate([cos_y, sin_y], axis=1)[order])
    reach = WIDEST * NZ // 96
    half = -(-(2 * reach + 1) // 64) * 64
    mode_kept = np.arange(half) - reach
    inside = mode_kept <= reach
    cos_k, sin_k = (part * inside for part in trig(np.arange(NZ), mode_kept, NZ))
    z_back = constant_halves(
        np.concatenate(
            [np.concatenate([cos_k, -sin_k], axis=1), np.concatenate([sin_k, cos_k], axis=1)], axis=0
        )
    )
    wave_kept = np.concatenate([TWO_PI / NZ * mode_kept * inside] * 2)
    wave_kept = jnp.asarray(np.broadcast_to(wave_kept, (8, 2 * half)), jnp.float32)
    cos_x, sin_x = trig(np.arange(NX), np.arange(KX), NX)
    weights = np.where(np.arange(KX) == 0, 1.0, 2.0)[None, :] * normalizer
    x_forward = constant_halves(
        np.stack(
            [
                np.concatenate([cos_x * weights, -sin_x * weights], axis=1),
                np.concatenate([-sin_x * weights, -cos_x * weights], axis=1),
            ]
        )
    )
    x_back = constant_halves(np.concatenate([cos_x.T, -sin_x.T], axis=0) * normalizer)

    params = pltpu.CompilerParams(vmem_limit_bytes=60 * 1024 * 1024)
    state_step = [
        pl.BlockSpec(
            (1, 2, slots, cols, 128),
            lambda i, k=k: (jnp.where(i < 4, i // 2 * 2, (i - 4) * 2 + 1), 0, 0, 0, k),
        )
        for k in range(width)
    ]
    state_w = [pl.BlockSpec((1, 2, slots, cols, 128), lambda i, k=k: (2, 0, 0, 0, k)) for k in range(width)]
    sent, sums = pl.pallas_call(
        functools.partial(forward_y, cols, slots, width, GMODES),
        grid=(FIELDS,),
        in_specs=state_step
        + state_w
        + [pl.BlockSpec((1, 2 * NY, NY), lambda i: (jnp.where(i < 4, i % 2, 0), 0, 0))] * 2,
        out_specs=[
            pl.BlockSpec((devices, rows_here, 1, cols, lanes), lambda i: (0, 0, i, 0, 0)),
            pl.BlockSpec((2 * groups_here, 8, 128), lambda i: (0, 0, 0)),
        ],
        out_shape=[
            jax.ShapeDtypeStruct((devices, rows_here, FIELDS, cols, lanes), jnp.float32),
            jax.ShapeDtypeStruct((2 * groups_here, 8, 128), jnp.float32),
        ],
        compiler_params=params,
        cost_estimate=pl.CostEstimate(
            flops=2 * 3 * FIELDS * 2 * NY * NY * cols * lanes, bytes_accessed=20 << 20, transcendentals=0
        ),
    )(*[state] * (2 * width), *y_forward)

    slot_mode = jnp.argsort(kz_group, stable=True).astype(jnp.int32)
    phase = slot_mode[:, None] * jnp.arange(NZ, dtype=jnp.int32)[None, :] % NZ
    theta = phase.astype(jnp.float32) * (TWO_PI / NZ)
    cos_z = jnp.cos(theta).reshape(groups, 1, slots, NZ)
    sin_z = jnp.sin(theta).reshape(groups, 1, slots, NZ)
    z_real = jnp.concatenate([cos_z, -sin_z], axis=1).reshape(2 * NZ, NZ)
    z_imag = jnp.concatenate([sin_z, cos_z], axis=1).reshape(2 * NZ, NZ)
    z_table = jnp.concatenate([z_real, z_imag], axis=1)
    z_high = lax.reduce_precision(z_table, 8, 7)
    z_low = (z_table - z_high).astype(jnp.bfloat16)
    z_high = z_high.astype(jnp.bfloat16)
    z_forward = (z_high, z_low)
    wave_slot = signed(slot_mode, NZ)
    wave_all = TWO_PI / NZ * wave_slot.astype(jnp.float32)
    wave_lanes = jnp.broadcast_to(wave_all.reshape(groups, 1, slots), (groups, 2, slots)).reshape(1, 2 * NZ)
    wave_lanes = jnp.broadcast_to(wave_lanes, (8, 2 * NZ))

    place = wave_slot + reach
    choose = (place[None, :] == jnp.arange(half, dtype=jnp.int32)[:, None]).reshape(half, groups, 1, slots)
    nothing = jnp.zeros_like(choose)
    choose = jnp.concatenate(
        [jnp.concatenate([choose, nothing], axis=2), jnp.concatenate([nothing, choose], axis=2)], axis=0
    )
    choose = choose.reshape(2 * half, 2 * NZ).astype(jnp.bfloat16)

    operands = [*z_forward, *x_forward, *x_back, *z_back, choose, wave_lanes, wave_kept, sums]
    final, totals = pl.pallas_call(
        functools.partial(travel, groups, slabs, TWO_PI / NX),
        in_specs=[pl.BlockSpec(memory_space=pl.ANY)] + [pl.BlockSpec(memory_space=pltpu.VMEM)] * len(operands),
        out_specs=[pl.BlockSpec(memory_space=pl.ANY)] * 2,
        out_shape=[
            jax.ShapeDtypeStruct((groups, rows_here, slabs, RETURNS, cols, lanes), jnp.float32),
            jax.ShapeDtypeStruct((slabs, *sums.shape), jnp.float32),
        ],
        scratch_shapes=[
            pltpu.VMEM((rows_here, devices, FIELDS, cols, lanes), jnp.float32),
            pltpu.VMEM((rows_here, slabs, RETURNS, cols, 2 * half), jnp.float32),
            pltpu.VMEM((rows_here, slabs, RETURNS, cols, 2 * half), jnp.float32),
            pltpu.VMEM((rows_here, groups, slabs, RETURNS, cols, lanes), jnp.float32),
        ]
        + [pltpu.SemaphoreType.DMA((rows_here,))] * 8
        + [pltpu.SemaphoreType.DMA] * 3,
        compiler_params=pltpu.CompilerParams(vmem_limit_bytes=63 * 1024 * 1024, has_side_effects=True),
    )(sent, *operands)

    means = jnp.sum(totals, axis=(0, 2, 3)).reshape(2, groups_here).T / (GMODES * KX * NY)
    power_here = lax.dynamic_slice_in_dim(power, grp_index * groups_here, groups_here)
    damping_here = lax.dynamic_slice_in_dim(damping, grp_index * groups_here, groups_here)
    forcing = (power_here - means[:, 0]) / (2.0 * (means[:, 1] + EPSILON))

    local_mode = signed(lax.dynamic_slice_in_dim(slot_mode, grp_index * slots, slots), NZ)
    mode_x = slab_index * cols + jnp.arange(cols, dtype=jnp.int32)
    mode_y = signed(jnp.arange(NY, dtype=jnp.int32), NY)
    zrow = jnp.stack(
        [
            TWO_PI / NZ * local_mode.astype(jnp.float32),
            (96 * jnp.abs(local_mode) <= cutoffs[2] * NZ).astype(jnp.float32),
            jnp.repeat(forcing, GMODES),
            jnp.repeat(damping_here, GMODES),
        ]
    )
    zrow = jnp.broadcast_to(zrow[:, :, None], (4, slots, NY))
    xrow = jnp.stack(
        [
            TWO_PI / NX * mode_x.astype(jnp.float32),
            (96 * mode_x <= cutoffs[0] * NX).astype(jnp.float32),
        ]
    )
    xrow = jnp.broadcast_to(xrow[:, :, None], (2, cols, NY))
    yrow = jnp.stack(
        [
            TWO_PI / NY * mode_y.astype(jnp.float32),
            (96 * jnp.abs(mode_y) <= cutoffs[1] * NY).astype(jnp.float32),
        ]
    )
    block = 8 if cols % 8 == 0 else cols
    return pl.pallas_call(
        functools.partial(finish, slots, 1, width),
        grid=(cols // block,),
        in_specs=[
            pl.BlockSpec((groups, rows_here, slabs, RETURNS, block, lanes), lambda i: (0, 0, 0, 0, i, 0))
        ]
        + [pl.BlockSpec((4, 2, slots, block, 128), lambda i, k=k: (0, 0, 0, i, k)) for k in range(width)]
        + [
            whole(y_back[0]),
            whole(y_back[1]),
            whole(zrow),
            pl.BlockSpec((2, block, NY), lambda i: (0, i, 0)),
            whole(yrow),
        ],
        out_specs=pl.BlockSpec((4, 2, slots, block, NY), lambda i: (0, 0, 0, i, 0)),
        out_shape=jax.ShapeDtypeStruct(state.shape, jnp.float32),
        scratch_shapes=[pltpu.VMEM((8 * slots * block, 128), jnp.float32)] * width,
        compiler_params=params,
        cost_estimate=pl.CostEstimate(flops=1 << 33, bytes_accessed=28 << 20, transcendentals=0),
    )(final, *[state] * width, *y_back, zrow, xrow, yrow)


def solution(mesh):
    return jax.shard_map(
        shards,
        mesh=mesh,
        in_specs=(P(None, None, "grp", "slab", None), P(), P(), P(), P()),
        out_specs=P(None, None, "grp", "slab", None),
        check_vma=False,
    )
```

```python
import functools
import math

import jax
import jax.numpy as jnp
import numpy as np
from jax import lax
from jax.experimental import pallas as pl
from jax.experimental.pallas import tpu as pltpu
from jax.sharding import PartitionSpec as P

TWO_PI = 6.283185307179586
TIME_STEP = 0.25
CORIOLIS = 1.0
BRUNT_SQUARED = 2.0
EPSILON = 1e-06
AHEAD = 3
LAG = 3
WIDEST = 32
FIELDS = 6
RETURNS = 5


def signed(index, length):
    return jnp.where(index < length // 2, index, index - length)


def halves(values):
    high = values.astype(jnp.bfloat16)
    low = (values - high.astype(jnp.float32)).astype(jnp.bfloat16)
    return high, low


def constant_halves(table):
    table = np.asarray(table, np.float32)
    high = table.astype(jnp.bfloat16)
    low = (table - high.astype(np.float32)).astype(jnp.bfloat16)
    return jnp.asarray(high), jnp.asarray(low)


def dot3(left, right, dims=(((1,), (0,)), ((), ()))):
    dot = functools.partial(lax.dot_general, dimension_numbers=dims, preferred_element_type=jnp.float32)
    return dot(left[0], right[0]) + (dot(left[0], right[1]) + dot(left[1], right[0]))


def trig(modes, points, length):
    phase = np.asarray(modes)[:, None] * np.asarray(points)[None, :] % length
    theta = phase * (2.0 * math.pi / length)
    return np.cos(theta), np.sin(theta)


def flat_rows(ref):
    shape = ref.shape
    return ref.reshape(math.prod(shape[:-1]), shape[-1])


def strided(ref, start, count, stride):
    return ref[pl.ds(start, count, stride=stride), :]


def forward_y(cols, slots, width, members, *refs):
    flow_w = [flat_rows(ref) for ref in refs[width : 2 * width]]
    high_ref, low_ref, out_ref, sums_ref = refs[2 * width :]
    out = flat_rows(out_ref)
    lanes = 2 * slots
    count = high_ref.shape[0]
    rows = [flat_rows(ref) for ref in refs[:width]]
    table = tuple(jnp.concatenate([ref[:, :count], ref[:, count:]], axis=0) for ref in (high_ref, low_ref))
    mode = signed(lax.broadcasted_iota(jnp.int32, (1, count), 1), count).astype(jnp.float32)
    sloped = (pl.program_id(0) == 1) | (pl.program_id(0) == 3)
    factor = jnp.where(sloped, TWO_PI / count * mode, 1.0)
    sign = jnp.where(lax.broadcasted_iota(jnp.int32, (1, lanes), 1) < slots, -1.0, 1.0)
    pair = 2 if cols % 2 == 0 else 1
    def some(first):
        taken = []
        for j in range(pair):
            for d in range(2):
                start = d * slots * cols + first + j
                taken.append(jnp.concatenate([strided(part, start, slots, cols) for part in rows], axis=1))
        data = halves(jnp.concatenate(taken, axis=0) * factor)
        both = dot3(table, data, (((1,), (1,)), ((), ())))
        for j in range(pair):
            part = both[:, j * lanes : (j + 1) * lanes]
            result = part[:count] + sign * pltpu.roll(part[count:], slots, 1)
            out[pl.ds(first + j, count, stride=cols), :] = result

    for i in range(cols // pair):
        some(i * pair)

    step = pl.program_id(0)
    here = sums_ref.shape[0] // 2
    size = members * cols

    @pl.when(step == 0)
    def _():
        sums_ref[...] = jnp.zeros_like(sums_ref)

    def add_up(which, one, two, weight):
        for group in range(here):
            for d in range(2):
                start = (d * slots + group * members) * cols
                for a, b in zip(one, two):
                    product = a[pl.ds(start, size), :] * b[pl.ds(start, size), :]
                    total = jnp.sum(product.reshape(size // 8, 8, 128), axis=0)
                    sums_ref[which * here + group] += weight * total

    @pl.when((step == 0) | (step == 2) | (step == 4))
    def _():
        add_up(1, rows, rows, 0.5)

    @pl.when(step == 5)
    def _():
        add_up(1, rows, rows, 0.5 / BRUNT_SQUARED)
        add_up(0, rows, flow_w, 1.0)


def planes(groups, slabs, x_step, read, zf_refs, xf_refs, xb_refs, zb_refs, kz_ref, kept_ref, write):
    wave_z = kz_ref[0:1, :]
    nz = zf_refs[0].shape[1] // 2
    u, u_y, w, w_y, v, b = (jnp.concatenate([read(g, f) for g in range(groups)], axis=1) for f in range(FIELDS))
    kx = u.shape[0]
    wave_x = x_step * lax.broadcasted_iota(jnp.int32, (kx, 1), 0).astype(jnp.float32)
    omega_x = w_y - wave_z * v
    omega_y = wave_z * u - wave_x * w
    omega_z = wave_x * v - u_y
    stacked = halves(jnp.concatenate([u, v, w, b, omega_x, omega_y, omega_z], axis=0))
    lines = dot3(stacked, (zf_refs[0][...], zf_refs[1][...]))
    grids = []
    for f in range(7):
        line = lines[f * kx : (f + 1) * kx]
        line = halves(jnp.concatenate([line[:, :nz], line[:, nz:]], axis=0))
        kind = 0 if f < 4 else 1
        grids.append(dot3((xf_refs[0][kind], xf_refs[1][kind]), line))
    gu, gv, gw, gb, gox, goy, goz = grids
    products = [gv * goz - gw * goy, gw * gox - gu * goz, gu * goy - gv * gox, gu * gb, gv * gb, gw * gb]
    table = (xb_refs[0][...], xb_refs[1][...])
    backs = []
    for product in products:
        back = dot3(table, halves(product))
        backs.append(jnp.concatenate([back[:kx], back[kx:]], axis=1))
    spectra = dot3(halves(jnp.concatenate(backs, axis=0)), (zb_refs[0][...], zb_refs[1][...]))
    hats = [spectra[f * kx : (f + 1) * kx] for f in range(6)]
    moved = wave_x * hats[3] + kept_ref[0:1, :] * hats[5]
    for f, hat in enumerate([hats[0], hats[1], hats[2], moved, hats[4]]):
        write(f, hat)


def slot_tables(members, reach, wide, group_ref, g, zf_refs, choose_ref, kz_ref, modes_ref):
    nz = group_ref.shape[1]
    slots = modes_ref.shape[0]
    half = choose_ref.shape[0] // 2
    rows = lax.broadcasted_iota(jnp.int32, (nz, nz), 0)
    lanes = lax.broadcasted_iota(jnp.int32, (nz, nz), 1)
    across = jnp.broadcast_to(group_ref[0:1, :], (nz, nz))
    down = across.T
    same = across == down
    rank_row = jnp.sum(jnp.where(same & (rows < lanes), 1.0, 0.0), axis=0, keepdims=True)
    rank_col = jnp.sum(jnp.where(same & (lanes < rows), 1.0, 0.0), axis=1, keepdims=True)
    place_row = across[0:1, :] * members + rank_row
    place_col = down[:, 0:1] * members + rank_col
    picks = jnp.where(rows.astype(jnp.float32) == place_row, 1.0, 0.0).astype(jnp.bfloat16)
    for part, out in zip(wide, zf_refs):
        chosen = jnp.dot(picks, part[...], preferred_element_type=jnp.float32)
        cosine, sine = chosen[:, :nz], chosen[:, nz:]
        for k in range(nz // slots):
            here = slice(k * slots, (k + 1) * slots)
            start = 2 * k * slots
            out[start : start + slots, :nz] = cosine[here].astype(jnp.bfloat16)
            out[start : start + slots, nz:] = sine[here].astype(jnp.bfloat16)
            out[start + slots : start + 2 * slots, :nz] = (-sine[here]).astype(jnp.bfloat16)
            out[start + slots : start + 2 * slots, nz:] = cosine[here].astype(jnp.bfloat16)
    lane = lax.broadcasted_iota(jnp.int32, (1, 2 * nz), 1)
    slot = (lane // (2 * slots) * slots + lane % slots).astype(jnp.float32)
    mode_col = signed(lax.broadcasted_iota(jnp.int32, (nz, 1), 0), nz).astype(jnp.float32)
    mode = jnp.sum(jnp.where(place_col == slot, mode_col, 0.0), axis=0, keepdims=True)
    kz_ref[...] = jnp.broadcast_to(TWO_PI / nz * mode, kz_ref.shape)
    part = (lane % (2 * slots) >= slots).astype(jnp.int32)
    row = lax.broadcasted_iota(jnp.int32, (half, 1), 0)
    hit = jnp.where((row - reach).astype(jnp.float32) == mode, 1.0, 0.0)
    for d in range(2):
        choose_ref[d * half : (d + 1) * half, :] = jnp.where(part == d, hit, 0.0).astype(jnp.bfloat16)
    mine = (lax.broadcasted_iota(jnp.int32, (slots, 1), 0) + g * slots).astype(jnp.float32)
    mode_row = signed(lax.broadcasted_iota(jnp.int32, (1, nz), 1), nz).astype(jnp.float32)
    own = jnp.sum(jnp.where(place_row == mine, mode_row, 0.0), axis=1, keepdims=True)
    modes_ref[...] = jnp.broadcast_to(own, modes_ref.shape)


def travel(groups, slabs, x_step, members, reach, *refs):
    (sent, wide0, wide1, xf0, xf1, xb0, xb1, zb0, zb1, group_ref, kept_ref, sums_ref, final, totals, modes) = refs[:15]
    zf0, zf1, choose, kz_ref = refs[15:19]
    (taken, made, kept, ready, f_send, f_recv, f_own, b_send, b_recv, c_send, c_recv, c_own, t_send, t_recv, t_own) = refs[19:]
    devices = groups * slabs
    count = taken.shape[0]
    cols, lanes = taken.shape[3:]
    ahead = min(AHEAD, count)
    lag = min(LAG, count)
    g = lax.axis_index("grp")
    s = lax.axis_index("slab")
    me = g * slabs + s

    def remote(source, target, send, recv, to_g, to_s):
        pltpu.make_async_remote_copy(
            src_ref=source,
            dst_ref=target,
            send_sem=send,
            recv_sem=recv,
            device_id={"grp": to_g, "slab": to_s},
            device_id_type=pl.DeviceIdType.MESH,
        ).start()

    def wait_all(ref, sem):
        pltpu.make_async_copy(ref, ref, sem).wait()

    def own_f(y):
        return pltpu.make_async_copy(sent.at[me, y], taken.at[y, me], f_own.at[y])

    def send_f(y):
        own_f(y).start()

        def one(k, carry):
            to = lax.rem(me + k, devices)
            remote(sent.at[to, y], taken.at[y, me], f_send.at[y], f_recv.at[y], to // slabs, lax.rem(to, slabs))
            return carry

        lax.fori_loop(1, devices, one, 0)

    def send_b(y):
        def one(k, carry):
            to = lax.rem(s + k, slabs)
            remote(made.at[y, to], kept.at[y, s], b_send.at[y], b_recv.at[y], g, to)
            return carry

        lax.fori_loop(1, slabs, one, 0)

    def own_c(y):
        return pltpu.make_async_copy(ready.at[y, g], final.at[g, :, y], c_own.at[y])

    def send_c(y):
        own_c(y).start()
        for k in range(1, groups):
            to = lax.rem(g + k, groups)
            remote(ready.at[y, to], final.at[g, :, y], c_send.at[y], c_recv.at[y], to, s)

    own_t = pltpu.make_async_copy(sums_ref, totals.at[s], t_own)

    def first(y, carry):
        send_f(y)
        return carry

    lax.fori_loop(0, ahead, first, 0)
    own_t.start()

    def send_t(k, carry):
        remote(sums_ref, totals.at[s], t_send, t_recv, g, lax.rem(s + k, slabs))
        return carry

    lax.fori_loop(1, slabs, send_t, 0)
    slot_tables(members, reach, (wide0, wide1), group_ref, g, (zf0, zf1), choose, kz_ref, modes)

    def step(t, carry):
        @pl.when(t < count)
        def _():
            own_f(t).wait()
            wait_all(taken.at[t, pl.ds(0, devices - 1)], f_recv.at[t])

            @pl.when(t + ahead < count)
            def _():
                send_f(t + ahead)

            def read(group, f):
                part = taken[t, group * slabs : (group + 1) * slabs, f]
                return part.reshape(slabs * cols, lanes)

            def write(f, value):
                made[t, :, f] = value.reshape(slabs, cols, value.shape[1])

            planes(
                groups, slabs, x_step, read, (zf0, zf1), (xf0, xf1), (xb0, xb1), (zb0, zb1), kz_ref, kept_ref, write
            )
            kept[t, s] = made[t, s]

        @pl.when(t >= lag)
        def _():
            y = t - lag
            wait_all(kept.at[y, pl.ds(0, slabs - 1)], b_recv.at[y])
            data = kept[y]
            high, low = halves(data.reshape(slabs * RETURNS * cols, data.shape[-1]))
            dot = functools.partial(jnp.dot, preferred_element_type=jnp.float32)
            picked = dot(high, choose[...]) + dot(low, choose[...])
            for group in range(groups):
                part = picked[:, group * lanes : (group + 1) * lanes]
                ready[y, group] = part.reshape(slabs, RETURNS, cols, lanes)

        @pl.when(t < count)
        def _():
            send_b(t)

        @pl.when(t >= lag)
        def _():
            send_c(t - lag)

        return carry

    lax.fori_loop(0, count + lag, step, 0)

    def last(y, carry):
        own_c(y).wait()
        wait_all(final.at[pl.ds(0, groups - 1), :, y], c_recv.at[y])
        wait_all(taken.at[y, pl.ds(0, devices - 1)], f_send.at[y])
        wait_all(kept.at[y, pl.ds(0, slabs - 1)], b_send.at[y])
        wait_all(ready.at[y, pl.ds(0, groups - 1)], c_send.at[y])
        return carry

    lax.fori_loop(0, count, last, 0)
    own_t.wait()
    wait_all(totals.at[pl.ds(0, slabs - 1)], t_recv)
    wait_all(totals.at[pl.ds(0, slabs - 1)], t_send)


def finish(slots, width, sizes, members, *refs):
    nx, ny, nz = sizes
    state_refs = refs[1 : width + 1]
    high_ref, low_ref, modes_ref, totals_ref, cutoffs_ref, damping_ref, power_ref, out_ref = refs[width + 1 : width + 9]
    out_parts = refs[width + 9 :]
    block = out_ref.shape[3]
    rows = flat_rows(refs[0])
    state = [flat_rows(ref) for ref in state_refs]
    table = (high_ref[...], low_ref[...])
    here = slots // members
    first_group = lax.axis_index("grp") * here
    x_count = pl.num_programs(0) * block
    first_x = lax.axis_index("slab") * x_count + pl.program_id(0) * block
    cells = members * (nx // 2) * ny
    sums = jnp.sum(totals_ref[...], axis=0)
    growths, dampings = [], []
    for group in range(here):
        flux, energy = (
            jnp.sum(jnp.sum(sums[k], axis=0, keepdims=True), axis=1, keepdims=True) / cells
            for k in (group, here + group)
        )
        forcing = (power_ref[first_group + group] - flux) / (2.0 * (energy + EPSILON))
        growths.append(jnp.broadcast_to(1.0 + TIME_STEP * forcing, (members, ny)))
        dampings.append(jnp.full((members, ny), damping_ref[first_group + group], jnp.float32))
    growth = jnp.concatenate(growths, axis=0)
    damping = jnp.concatenate(dampings, axis=0)
    mode_z = jnp.concatenate([modes_ref[...]] * width, axis=1)
    wave_z = TWO_PI / nz * mode_z
    mode_y = signed(lax.broadcasted_iota(jnp.int32, (1, ny), 1), ny).astype(jnp.float32)
    wave_y = TWO_PI / ny * mode_y

    def within(mode, which, length):
        limit = (cutoffs_ref[which] * length).astype(jnp.float32)
        return jnp.where(96.0 * jnp.abs(mode) <= limit, 1.0, 0.0)

    kept_yz = within(mode_z, 2, nz) * within(mode_y, 1, ny) * TIME_STEP

    def load(c, d, x):
        start = (c * 2 + d) * slots * block + x
        return jnp.concatenate([strided(part, start, slots, block) for part in state], axis=1)

    def store(c, d, x, value):
        start = (c * 2 + d) * slots * block + x
        for k in range(width):
            out_parts[k][pl.ds(start, slots, stride=block), :] = value[:, 128 * k : 128 * (k + 1)]

    def one(x):
        columns = [rows[pl.ds(f * block + x, ny, stride=RETURNS * block), :].T for f in range(RETURNS)]
        both = dot3(halves(jnp.concatenate(columns, axis=0)), table)
        tends = []
        for f in range(RETURNS):
            re = both[2 * f * slots : (2 * f + 1) * slots]
            im = both[(2 * f + 1) * slots : (2 * f + 2) * slots]
            tends.append((re[:, :ny] + im[:, ny:], im[:, :ny] - re[:, ny:]))
        mode_x = jnp.full((1, ny), (first_x + x).astype(jnp.float32), jnp.float32)
        wave_x = TWO_PI / nx * mode_x
        kept = kept_yz * within(mode_x, 0, nx)
        wave_sq = wave_x * wave_x + wave_y * wave_y + wave_z * wave_z
        implicit = 1.0 + TIME_STEP * damping * wave_sq
        rotation = TIME_STEP * CORIOLIS
        first = 1.0 / (implicit * implicit + rotation * rotation)
        second = 1.0 / (implicit * implicit + TIME_STEP * TIME_STEP * BRUNT_SQUARED)
        inverse_sq = 1.0 / (wave_sq + (wave_sq == 0).astype(jnp.float32))
        total = [tends[3][d] + wave_y * tends[4][d] for d in range(2)]
        source = [total[1], -total[0]]
        for d in range(2):
            right_x = growth * load(0, d, x) + kept * tends[0][d]
            right_y = growth * load(1, d, x) + kept * tends[1][d]
            right_z = growth * load(2, d, x) + kept * tends[2][d]
            right_b = load(3, d, x) + kept * source[d]
            new_x = (implicit * right_x + rotation * right_y) * first
            new_y = (implicit * right_y - rotation * right_x) * first
            new_z = (implicit * right_z + TIME_STEP * right_b) * second
            new_b = (implicit * right_b - TIME_STEP * BRUNT_SQUARED * right_z) * second
            inner = (wave_x * new_x + wave_y * new_y + wave_z * new_z) * inverse_sq
            store(0, d, x, new_x - wave_x * inner)
            store(1, d, x, new_y - wave_y * inner)
            store(2, d, x, new_z - wave_z * inner)
            store(3, d, x, new_b)

    unrolled = 2 if block % 2 == 0 else 1

    def some(i, carry):
        for k in range(unrolled):
            one(i * unrolled + k)
        return carry

    lax.fori_loop(0, block // unrolled, some, 0)
    for k in range(width):
        for c in range(4):
            for d in range(2):
                size = slots * block
                part = out_parts[k][(c * 2 + d) * size : (c * 2 + d + 1) * size, :]
                out_ref[c, d, :, :, 128 * k : 128 * (k + 1)] = part.reshape(slots, block, 128)


def whole(array):
    return pl.BlockSpec(array.shape, lambda *_: (0,) * array.ndim)


def shards(state, kz_group, cutoffs, damping, power):
    groups = lax.axis_size("grp")
    slabs = lax.axis_size("slab")
    slots = state.shape[2]
    cols = state.shape[3]
    NY = state.shape[4]
    NZ = slots * groups
    KX = cols * slabs
    NX = 2 * KX
    GROUPS = damping.shape[0]
    GMODES = NZ // GROUPS
    devices = groups * slabs
    rows_here = NY // devices
    groups_here = GROUPS // groups
    lanes = 2 * slots
    width = NY // 128
    normalizer = 1.0 / math.sqrt(NX * NY * NZ)

    wide_y = constant_halves(np.concatenate(trig(np.arange(NY), np.arange(NY), NY), axis=1))
    wide_z = wide_y
    if NZ != NY:
        wide_z = constant_halves(np.concatenate(trig(np.arange(NZ), np.arange(NZ), NZ), axis=1))
    reach = WIDEST * NZ // 96
    half = -(-(2 * reach + 1) // 64) * 64
    mode_kept = np.arange(half) - reach
    inside = mode_kept <= reach
    cos_k, sin_k = (part * inside for part in trig(np.arange(NZ), mode_kept, NZ))
    z_back = constant_halves(
        np.concatenate(
            [np.concatenate([cos_k, -sin_k], axis=1), np.concatenate([sin_k, cos_k], axis=1)], axis=0
        )
    )
    wave_kept = np.concatenate([TWO_PI / NZ * mode_kept * inside] * 2)
    wave_kept = jnp.asarray(np.broadcast_to(wave_kept, (8, 2 * half)), jnp.float32)
    cos_x, sin_x = trig(np.arange(NX), np.arange(KX), NX)
    weights = np.where(np.arange(KX) == 0, 1.0, 2.0)[None, :] * normalizer
    x_forward = constant_halves(
        np.stack(
            [
                np.concatenate([cos_x * weights, -sin_x * weights], axis=1),
                np.concatenate([-sin_x * weights, -cos_x * weights], axis=1),
            ]
        )
    )
    x_back = constant_halves(np.concatenate([cos_x.T, -sin_x.T], axis=0) * normalizer)

    params = pltpu.CompilerParams(vmem_limit_bytes=60 * 1024 * 1024)
    state_step = [
        pl.BlockSpec(
            (1, 2, slots, cols, 128),
            lambda i, k=k: (jnp.where(i < 4, i // 2 * 2, (i - 4) * 2 + 1), 0, 0, 0, k),
        )
        for k in range(width)
    ]
    state_w = [pl.BlockSpec((1, 2, slots, cols, 128), lambda i, k=k: (2, 0, 0, 0, k)) for k in range(width)]
    sent, sums = pl.pallas_call(
        functools.partial(forward_y, cols, slots, width, GMODES),
        grid=(FIELDS,),
        in_specs=state_step
        + state_w
        + [whole(part) for part in wide_y],
        out_specs=[
            pl.BlockSpec((devices, rows_here, 1, cols, lanes), lambda i: (0, 0, i, 0, 0)),
            pl.BlockSpec((2 * groups_here, 8, 128), lambda i: (0, 0, 0)),
        ],
        out_shape=[
            jax.ShapeDtypeStruct((devices, rows_here, FIELDS, cols, lanes), jnp.float32),
            jax.ShapeDtypeStruct((2 * groups_here, 8, 128), jnp.float32),
        ],
        compiler_params=params,
        cost_estimate=pl.CostEstimate(
            flops=2 * 3 * FIELDS * 2 * NY * NY * cols * lanes, bytes_accessed=20 << 20, transcendentals=0
        ),
    )(*[state] * (2 * width), *wide_y)

    group_row = jnp.broadcast_to(kz_group[None, :].astype(jnp.float32), (8, NZ))
    operands = [*wide_z, *x_forward, *x_back, *z_back, group_row, wave_kept, sums]
    final, totals, modes = pl.pallas_call(
        functools.partial(travel, groups, slabs, TWO_PI / NX, GMODES, reach),
        in_specs=[pl.BlockSpec(memory_space=pl.ANY)] + [pl.BlockSpec(memory_space=pltpu.VMEM)] * len(operands),
        out_specs=[pl.BlockSpec(memory_space=pl.ANY)] * 2 + [pl.BlockSpec(memory_space=pltpu.VMEM)],
        out_shape=[
            jax.ShapeDtypeStruct((groups, slabs, rows_here, RETURNS, cols, lanes), jnp.float32),
            jax.ShapeDtypeStruct((slabs, *sums.shape), jnp.float32),
            jax.ShapeDtypeStruct((slots, 128), jnp.float32),
        ],
        scratch_shapes=[
            pltpu.VMEM((2 * NZ, 2 * NZ), jnp.bfloat16),
            pltpu.VMEM((2 * NZ, 2 * NZ), jnp.bfloat16),
            pltpu.VMEM((2 * half, 2 * NZ), jnp.bfloat16),
            pltpu.VMEM((8, 2 * NZ), jnp.float32),
            pltpu.VMEM((rows_here, devices, FIELDS, cols, lanes), jnp.float32),
            pltpu.VMEM((rows_here, slabs, RETURNS, cols, 2 * half), jnp.float32),
            pltpu.VMEM((rows_here, slabs, RETURNS, cols, 2 * half), jnp.float32),
            pltpu.VMEM((rows_here, groups, slabs, RETURNS, cols, lanes), jnp.float32),
        ]
        + [pltpu.SemaphoreType.DMA((rows_here,))] * 8
        + [pltpu.SemaphoreType.DMA] * 3,
        compiler_params=pltpu.CompilerParams(vmem_limit_bytes=63 * 1024 * 1024, has_side_effects=True),
    )(sent, *operands)

    block = 8 if cols % 8 == 0 else cols
    return pl.pallas_call(
        functools.partial(finish, slots, width, (NX, NY, NZ), GMODES),
        grid=(cols // block,),
        in_specs=[pl.BlockSpec((groups, slabs, rows_here, RETURNS, block, lanes), lambda i: (0, 0, 0, 0, i, 0))]
        + [pl.BlockSpec((4, 2, slots, block, 128), lambda i, k=k: (0, 0, 0, i, k)) for k in range(width)]
        + [whole(wide_y[0]), whole(wide_y[1]), whole(modes), whole(totals)]
        + [pl.BlockSpec(memory_space=pltpu.SMEM)] * 3,
        out_specs=pl.BlockSpec((4, 2, slots, block, NY), lambda i: (0, 0, 0, i, 0)),
        out_shape=jax.ShapeDtypeStruct(state.shape, jnp.float32),
        scratch_shapes=[pltpu.VMEM((8 * slots * block, 128), jnp.float32)] * width,
        compiler_params=params,
        cost_estimate=pl.CostEstimate(flops=1 << 33, bytes_accessed=28 << 20, transcendentals=0),
    )(final, *[state] * width, *wide_y, modes, totals, cutoffs, damping, power)


def solution(mesh):
    return jax.shard_map(
        shards,
        mesh=mesh,
        in_specs=(P(None, None, "grp", "slab", None), P(), P(), P(), P()),
        out_specs=P(None, None, "grp", "slab", None),
        check_vma=False,
    )
```

```python
import functools
import math

import jax
import jax.numpy as jnp
import numpy as np
from jax import lax
from jax.experimental import pallas as pl
from jax.experimental.pallas import tpu as pltpu
from jax.sharding import PartitionSpec as P

TWO_PI = 6.283185307179586
TIME_STEP = 0.25
CORIOLIS = 1.0
BRUNT_SQUARED = 2.0
EPSILON = 1e-06
AHEAD = 3
LAG = 3
PARTS = ((0, 3), (3, 5))
WIDEST = 32
FIELDS = 6
RETURNS = 5


def signed(index, length):
    return jnp.where(index < length // 2, index, index - length)


def halves(values):
    high = values.astype(jnp.bfloat16)
    low = (values - high.astype(jnp.float32)).astype(jnp.bfloat16)
    return high, low


def constant_halves(table):
    table = np.asarray(table, np.float32)
    high = table.astype(jnp.bfloat16)
    low = (table - high.astype(np.float32)).astype(jnp.bfloat16)
    return jnp.asarray(high), jnp.asarray(low)


def dot3(left, right, dims=(((1,), (0,)), ((), ()))):
    dot = functools.partial(lax.dot_general, dimension_numbers=dims, preferred_element_type=jnp.float32)
    return dot(left[0], right[0]) + (dot(left[0], right[1]) + dot(left[1], right[0]))


def trig(modes, points, length):
    phase = np.asarray(modes)[:, None] * np.asarray(points)[None, :] % length
    theta = phase * (2.0 * math.pi / length)
    return np.cos(theta), np.sin(theta)


def flat_rows(ref):
    shape = ref.shape
    return ref.reshape(math.prod(shape[:-1]), shape[-1])


def strided(ref, start, count, stride):
    return ref[pl.ds(start, count, stride=stride), :]


def forward_y(cols, slots, width, members, *refs):
    flow_w = [flat_rows(ref) for ref in refs[width : 2 * width]]
    high_ref, low_ref, out_ref, sums_ref = refs[2 * width :]
    out = flat_rows(out_ref)
    lanes = 2 * slots
    count = high_ref.shape[0]
    rows = [flat_rows(ref) for ref in refs[:width]]
    table = tuple(jnp.concatenate([ref[:, :count], ref[:, count:]], axis=0) for ref in (high_ref, low_ref))
    mode = signed(lax.broadcasted_iota(jnp.int32, (1, count), 1), count).astype(jnp.float32)
    sloped = (pl.program_id(0) == 1) | (pl.program_id(0) == 3)
    factor = jnp.where(sloped, TWO_PI / count * mode, 1.0)
    sign = jnp.where(lax.broadcasted_iota(jnp.int32, (1, lanes), 1) < slots, -1.0, 1.0)
    pair = 2 if cols % 2 == 0 else 1
    def some(first):
        taken = []
        for j in range(pair):
            for d in range(2):
                start = d * slots * cols + first + j
                taken.append(jnp.concatenate([strided(part, start, slots, cols) for part in rows], axis=1))
        data = halves(jnp.concatenate(taken, axis=0) * factor)
        both = dot3(table, data, (((1,), (1,)), ((), ())))
        for j in range(pair):
            part = both[:, j * lanes : (j + 1) * lanes]
            result = part[:count] + sign * pltpu.roll(part[count:], slots, 1)
            out[pl.ds(first + j, count, stride=cols), :] = result

    for i in range(cols // pair):
        some(i * pair)

    step = pl.program_id(0)
    here = sums_ref.shape[0] // 2
    size = members * cols

    @pl.when(step == 0)
    def _():
        sums_ref[...] = jnp.zeros_like(sums_ref)

    def add_up(which, one, two, weight):
        for group in range(here):
            for d in range(2):
                start = (d * slots + group * members) * cols
                for a, b in zip(one, two):
                    product = a[pl.ds(start, size), :] * b[pl.ds(start, size), :]
                    total = jnp.sum(product.reshape(size // 8, 8, 128), axis=0)
                    sums_ref[which * here + group] += weight * total

    @pl.when((step == 0) | (step == 2) | (step == 4))
    def _():
        add_up(1, rows, rows, 0.5)

    @pl.when(step == 5)
    def _():
        add_up(1, rows, rows, 0.5 / BRUNT_SQUARED)
        add_up(0, rows, flow_w, 1.0)


def planes(groups, slabs, x_step, read, zf_refs, xf_refs, xb_refs, zb_refs, kz_ref, kept_ref, write):
    wave_z = kz_ref[0:1, :]
    nz = zf_refs[0].shape[1] // 2
    u, u_y, w, w_y, v, b = (jnp.concatenate([read(g, f) for g in range(groups)], axis=1) for f in range(FIELDS))
    kx = u.shape[0]
    wave_x = x_step * lax.broadcasted_iota(jnp.int32, (kx, 1), 0).astype(jnp.float32)
    omega_x = w_y - wave_z * v
    omega_y = wave_z * u - wave_x * w
    omega_z = wave_x * v - u_y
    stacked = halves(jnp.concatenate([u, v, w, b, omega_x, omega_y, omega_z], axis=0))
    lines = dot3(stacked, (zf_refs[0][...], zf_refs[1][...]))
    grids = []
    for f in range(7):
        line = lines[f * kx : (f + 1) * kx]
        line = halves(jnp.concatenate([line[:, :nz], line[:, nz:]], axis=0))
        kind = 0 if f < 4 else 1
        grids.append(dot3((xf_refs[0][kind], xf_refs[1][kind]), line))
    gu, gv, gw, gb, gox, goy, goz = grids
    products = [gv * goz - gw * goy, gw * gox - gu * goz, gu * goy - gv * gox, gu * gb, gv * gb, gw * gb]
    table = (xb_refs[0][...], xb_refs[1][...])
    backs = []
    for product in products:
        back = dot3(table, halves(product))
        backs.append(jnp.concatenate([back[:kx], back[kx:]], axis=1))
    spectra = dot3(halves(jnp.concatenate(backs, axis=0)), (zb_refs[0][...], zb_refs[1][...]))
    hats = [spectra[f * kx : (f + 1) * kx] for f in range(6)]
    moved = wave_x * hats[3] + kept_ref[0:1, :] * hats[5]
    for f, hat in enumerate([hats[0], hats[1], hats[2], moved, hats[4]]):
        write(f, hat)


def slot_tables(members, reach, wide, group_ref, g, zf_refs, choose_ref, kz_ref, modes_ref):
    nz = group_ref.shape[1]
    slots = modes_ref.shape[0]
    half = choose_ref.shape[0] // 2
    rows = lax.broadcasted_iota(jnp.int32, (nz, nz), 0)
    lanes = lax.broadcasted_iota(jnp.int32, (nz, nz), 1)
    across = jnp.broadcast_to(group_ref[0:1, :], (nz, nz))
    down = across.T
    same = across == down
    rank_row = jnp.sum(jnp.where(same & (rows < lanes), 1.0, 0.0), axis=0, keepdims=True)
    rank_col = jnp.sum(jnp.where(same & (lanes < rows), 1.0, 0.0), axis=1, keepdims=True)
    place_row = across[0:1, :] * members + rank_row
    place_col = down[:, 0:1] * members + rank_col
    picks = jnp.where(rows.astype(jnp.float32) == place_row, 1.0, 0.0).astype(jnp.bfloat16)
    for part, out in zip(wide, zf_refs):
        chosen = jnp.dot(picks, part[...], preferred_element_type=jnp.float32)
        cosine, sine = chosen[:, :nz], chosen[:, nz:]
        for k in range(nz // slots):
            here = slice(k * slots, (k + 1) * slots)
            start = 2 * k * slots
            out[start : start + slots, :nz] = cosine[here].astype(jnp.bfloat16)
            out[start : start + slots, nz:] = sine[here].astype(jnp.bfloat16)
            out[start + slots : start + 2 * slots, :nz] = (-sine[here]).astype(jnp.bfloat16)
            out[start + slots : start + 2 * slots, nz:] = cosine[here].astype(jnp.bfloat16)
    lane = lax.broadcasted_iota(jnp.int32, (1, 2 * nz), 1)
    slot = (lane // (2 * slots) * slots + lane % slots).astype(jnp.float32)
    mode_col = signed(lax.broadcasted_iota(jnp.int32, (nz, 1), 0), nz).astype(jnp.float32)
    mode = jnp.sum(jnp.where(place_col == slot, mode_col, 0.0), axis=0, keepdims=True)
    kz_ref[...] = jnp.broadcast_to(TWO_PI / nz * mode, kz_ref.shape)
    part = (lane % (2 * slots) >= slots).astype(jnp.int32)
    row = lax.broadcasted_iota(jnp.int32, (half, 1), 0)
    hit = jnp.where((row - reach).astype(jnp.float32) == mode, 1.0, 0.0)
    for d in range(2):
        choose_ref[d * half : (d + 1) * half, :] = jnp.where(part == d, hit, 0.0).astype(jnp.bfloat16)
    mine = (lax.broadcasted_iota(jnp.int32, (slots, 1), 0) + g * slots).astype(jnp.float32)
    mode_row = signed(lax.broadcasted_iota(jnp.int32, (1, nz), 1), nz).astype(jnp.float32)
    own = jnp.sum(jnp.where(place_row == mine, mode_row, 0.0), axis=1, keepdims=True)
    modes_ref[...] = jnp.broadcast_to(own, modes_ref.shape)


def travel(groups, slabs, x_step, members, reach, *refs):
    (sent, wide0, wide1, xf0, xf1, xb0, xb1, zb0, zb1, group_ref, kept_ref, sums_ref, final, totals, modes) = refs[:15]
    zf0, zf1, choose, kz_ref = refs[15:19]
    (taken, made, kept, ready, f_send, f_recv, f_own, b_send, b_recv, c_send, c_recv, c_own, t_send, t_recv, t_own) = refs[19:]
    devices = groups * slabs
    count = taken.shape[0]
    cols, lanes = taken.shape[3:]
    ahead = min(AHEAD, count)
    lag = min(LAG, count)
    g = lax.axis_index("grp")
    s = lax.axis_index("slab")
    me = g * slabs + s

    def remote(source, target, send, recv, to_g, to_s):
        pltpu.make_async_remote_copy(
            src_ref=source,
            dst_ref=target,
            send_sem=send,
            recv_sem=recv,
            device_id={"grp": to_g, "slab": to_s},
            device_id_type=pl.DeviceIdType.MESH,
        ).start()

    def wait_all(ref, sem):
        pltpu.make_async_copy(ref, ref, sem).wait()

    def own_f(y):
        return pltpu.make_async_copy(sent.at[me, y], taken.at[y, me], f_own.at[y])

    def send_f(y):
        own_f(y).start()

        def one(k, carry):
            to = lax.rem(me + k, devices)
            remote(sent.at[to, y], taken.at[y, me], f_send.at[y], f_recv.at[y], to // slabs, lax.rem(to, slabs))
            return carry

        lax.fori_loop(1, devices, one, 0)

    parts = len(PARTS)

    def send_b(y):
        for p, (low, high) in enumerate(PARTS):
            fields = pl.ds(low, high - low)

            def one(k, carry):
                to = lax.rem(s + k, slabs)
                q = y * parts + p
                remote(made.at[y, to, fields], kept.at[y, s, fields], b_send.at[q], b_recv.at[q], g, to)
                return carry

            lax.fori_loop(1, slabs, one, 0)

    def own_c(y, p):
        fields = pl.ds(PARTS[p][0], PARTS[p][1] - PARTS[p][0])
        return pltpu.make_async_copy(ready.at[y, g, :, fields], final.at[g, :, y, fields], c_own.at[y * parts + p])

    def send_c(y, p):
        own_c(y, p).start()
        fields = pl.ds(PARTS[p][0], PARTS[p][1] - PARTS[p][0])
        q = y * parts + p
        for k in range(1, groups):
            to = lax.rem(g + k, groups)
            remote(ready.at[y, to, :, fields], final.at[g, :, y, fields], c_send.at[q], c_recv.at[q], to, s)

    def back(y, p):
        low, high = PARTS[p]
        size = high - low
        wait_all(kept.at[y, pl.ds(0, slabs - 1), pl.ds(low, size)], b_recv.at[y * parts + p])
        data = kept[y, :, low:high]
        upper, lower = halves(data.reshape(slabs * size * cols, data.shape[-1]))
        dot = functools.partial(jnp.dot, preferred_element_type=jnp.float32)
        picked = dot(upper, choose[...]) + dot(lower, choose[...])
        for group in range(groups):
            part = picked[:, group * lanes : (group + 1) * lanes]
            ready[y, group, :, low:high] = part.reshape(slabs, size, cols, lanes)

    own_t = pltpu.make_async_copy(sums_ref, totals.at[s], t_own)

    def first(y, carry):
        send_f(y)
        return carry

    lax.fori_loop(0, ahead, first, 0)
    own_t.start()

    def send_t(k, carry):
        remote(sums_ref, totals.at[s], t_send, t_recv, g, lax.rem(s + k, slabs))
        return carry

    lax.fori_loop(1, slabs, send_t, 0)
    slot_tables(members, reach, (wide0, wide1), group_ref, g, (zf0, zf1), choose, kz_ref, modes)

    def step(t, carry):
        @pl.when(t < count)
        def _():
            own_f(t).wait()
            wait_all(taken.at[t, pl.ds(0, devices - 1)], f_recv.at[t])

            @pl.when(t + ahead < count)
            def _():
                send_f(t + ahead)

            def read(group, f):
                part = taken[t, group * slabs : (group + 1) * slabs, f]
                return part.reshape(slabs * cols, lanes)

            def write(f, value):
                made[t, :, f] = value.reshape(slabs, cols, value.shape[1])

            planes(
                groups, slabs, x_step, read, (zf0, zf1), (xf0, xf1), (xb0, xb1), (zb0, zb1), kz_ref, kept_ref, write
            )
            kept[t, s] = made[t, s]

        @pl.when(t >= lag)
        def _():
            back(t - lag, 0)

        @pl.when(t < count)
        def _():
            send_b(t)

        @pl.when(t >= lag)
        def _():
            send_c(t - lag, 0)
            for p in range(1, parts):
                back(t - lag, p)
                send_c(t - lag, p)

        return carry

    lax.fori_loop(0, count + lag, step, 0)

    def last(y, carry):
        wait_all(taken.at[y, pl.ds(0, devices - 1)], f_send.at[y])
        for p, (low, high) in enumerate(PARTS):
            fields = pl.ds(low, high - low)
            q = y * parts + p
            own_c(y, p).wait()
            wait_all(final.at[pl.ds(0, groups - 1), :, y, fields], c_recv.at[q])
            wait_all(kept.at[y, pl.ds(0, slabs - 1), fields], b_send.at[q])
            wait_all(ready.at[y, pl.ds(0, groups - 1), :, fields], c_send.at[q])
        return carry

    lax.fori_loop(0, count, last, 0)
    own_t.wait()
    wait_all(totals.at[pl.ds(0, slabs - 1)], t_recv)
    wait_all(totals.at[pl.ds(0, slabs - 1)], t_send)


def finish(slots, width, sizes, members, *refs):
    nx, ny, nz = sizes
    state_refs = refs[1 : width + 1]
    high_ref, low_ref, modes_ref, totals_ref, cutoffs_ref, damping_ref, power_ref, out_ref = refs[width + 1 : width + 9]
    out_parts = refs[width + 9 :]
    block = out_ref.shape[3]
    rows = flat_rows(refs[0])
    state = [flat_rows(ref) for ref in state_refs]
    table = (high_ref[...], low_ref[...])
    here = slots // members
    first_group = lax.axis_index("grp") * here
    x_count = pl.num_programs(0) * block
    first_x = lax.axis_index("slab") * x_count + pl.program_id(0) * block
    cells = members * (nx // 2) * ny
    sums = jnp.sum(totals_ref[...], axis=0)
    growths, dampings = [], []
    for group in range(here):
        flux, energy = (
            jnp.sum(jnp.sum(sums[k], axis=0, keepdims=True), axis=1, keepdims=True) / cells
            for k in (group, here + group)
        )
        forcing = (power_ref[first_group + group] - flux) / (2.0 * (energy + EPSILON))
        growths.append(jnp.broadcast_to(1.0 + TIME_STEP * forcing, (members, ny)))
        dampings.append(jnp.full((members, ny), damping_ref[first_group + group], jnp.float32))
    growth = jnp.concatenate(growths, axis=0)
    damping = jnp.concatenate(dampings, axis=0)
    mode_z = jnp.concatenate([modes_ref[...]] * width, axis=1)
    wave_z = TWO_PI / nz * mode_z
    mode_y = signed(lax.broadcasted_iota(jnp.int32, (1, ny), 1), ny).astype(jnp.float32)
    wave_y = TWO_PI / ny * mode_y

    def within(mode, which, length):
        limit = (cutoffs_ref[which] * length).astype(jnp.float32)
        return jnp.where(96.0 * jnp.abs(mode) <= limit, 1.0, 0.0)

    kept_yz = within(mode_z, 2, nz) * within(mode_y, 1, ny) * TIME_STEP

    def load(c, d, x):
        start = (c * 2 + d) * slots * block + x
        return jnp.concatenate([strided(part, start, slots, block) for part in state], axis=1)

    def store(c, d, x, value):
        start = (c * 2 + d) * slots * block + x
        for k in range(width):
            out_parts[k][pl.ds(start, slots, stride=block), :] = value[:, 128 * k : 128 * (k + 1)]

    def one(x):
        columns = [rows[pl.ds(f * block + x, ny, stride=RETURNS * block), :].T for f in range(RETURNS)]
        both = dot3(halves(jnp.concatenate(columns, axis=0)), table)
        tends = []
        for f in range(RETURNS):
            re = both[2 * f * slots : (2 * f + 1) * slots]
            im = both[(2 * f + 1) * slots : (2 * f + 2) * slots]
            tends.append((re[:, :ny] + im[:, ny:], im[:, :ny] - re[:, ny:]))
        mode_x = jnp.full((1, ny), (first_x + x).astype(jnp.float32), jnp.float32)
        wave_x = TWO_PI / nx * mode_x
        kept = kept_yz * within(mode_x, 0, nx)
        wave_sq = wave_x * wave_x + wave_y * wave_y + wave_z * wave_z
        implicit = 1.0 + TIME_STEP * damping * wave_sq
        rotation = TIME_STEP * CORIOLIS
        first = 1.0 / (implicit * implicit + rotation * rotation)
        second = 1.0 / (implicit * implicit + TIME_STEP * TIME_STEP * BRUNT_SQUARED)
        inverse_sq = 1.0 / (wave_sq + (wave_sq == 0).astype(jnp.float32))
        total = [tends[3][d] + wave_y * tends[4][d] for d in range(2)]
        source = [total[1], -total[0]]
        for d in range(2):
            right_x = growth * load(0, d, x) + kept * tends[0][d]
            right_y = growth * load(1, d, x) + kept * tends[1][d]
            right_z = growth * load(2, d, x) + kept * tends[2][d]
            right_b = load(3, d, x) + kept * source[d]
            new_x = (implicit * right_x + rotation * right_y) * first
            new_y = (implicit * right_y - rotation * right_x) * first
            new_z = (implicit * right_z + TIME_STEP * right_b) * second
            new_b = (implicit * right_b - TIME_STEP * BRUNT_SQUARED * right_z) * second
            inner = (wave_x * new_x + wave_y * new_y + wave_z * new_z) * inverse_sq
            store(0, d, x, new_x - wave_x * inner)
            store(1, d, x, new_y - wave_y * inner)
            store(2, d, x, new_z - wave_z * inner)
            store(3, d, x, new_b)

    unrolled = 4 if block % 4 == 0 else 1

    def some(i, carry):
        for k in range(unrolled):
            one(i * unrolled + k)
        return carry

    lax.fori_loop(0, block // unrolled, some, 0)
    for k in range(width):
        for c in range(4):
            for d in range(2):
                size = slots * block
                part = out_parts[k][(c * 2 + d) * size : (c * 2 + d + 1) * size, :]
                out_ref[c, d, :, :, 128 * k : 128 * (k + 1)] = part.reshape(slots, block, 128)


def whole(array):
    return pl.BlockSpec(array.shape, lambda *_: (0,) * array.ndim)


def shards(state, kz_group, cutoffs, damping, power):
    groups = lax.axis_size("grp")
    slabs = lax.axis_size("slab")
    slots = state.shape[2]
    cols = state.shape[3]
    NY = state.shape[4]
    NZ = slots * groups
    KX = cols * slabs
    NX = 2 * KX
    GROUPS = damping.shape[0]
    GMODES = NZ // GROUPS
    devices = groups * slabs
    rows_here = NY // devices
    groups_here = GROUPS // groups
    lanes = 2 * slots
    width = NY // 128
    normalizer = 1.0 / math.sqrt(NX * NY * NZ)

    wide_y = constant_halves(np.concatenate(trig(np.arange(NY), np.arange(NY), NY), axis=1))
    wide_z = wide_y
    if NZ != NY:
        wide_z = constant_halves(np.concatenate(trig(np.arange(NZ), np.arange(NZ), NZ), axis=1))
    reach = WIDEST * NZ // 96
    half = -(-(2 * reach + 1) // 64) * 64
    mode_kept = np.arange(half) - reach
    inside = mode_kept <= reach
    cos_k, sin_k = (part * inside for part in trig(np.arange(NZ), mode_kept, NZ))
    z_back = constant_halves(
        np.concatenate(
            [np.concatenate([cos_k, -sin_k], axis=1), np.concatenate([sin_k, cos_k], axis=1)], axis=0
        )
    )
    wave_kept = np.concatenate([TWO_PI / NZ * mode_kept * inside] * 2)
    wave_kept = jnp.asarray(np.broadcast_to(wave_kept, (8, 2 * half)), jnp.float32)
    cos_x, sin_x = trig(np.arange(NX), np.arange(KX), NX)
    weights = np.where(np.arange(KX) == 0, 1.0, 2.0)[None, :] * normalizer
    x_forward = constant_halves(
        np.stack(
            [
                np.concatenate([cos_x * weights, -sin_x * weights], axis=1),
                np.concatenate([-sin_x * weights, -cos_x * weights], axis=1),
            ]
        )
    )
    x_back = constant_halves(np.concatenate([cos_x.T, -sin_x.T], axis=0) * normalizer)

    params = pltpu.CompilerParams(vmem_limit_bytes=60 * 1024 * 1024)
    state_step = [
        pl.BlockSpec(
            (1, 2, slots, cols, 128),
            lambda i, k=k: (jnp.where(i < 4, i // 2 * 2, (i - 4) * 2 + 1), 0, 0, 0, k),
        )
        for k in range(width)
    ]
    state_w = [pl.BlockSpec((1, 2, slots, cols, 128), lambda i, k=k: (2, 0, 0, 0, k)) for k in range(width)]
    sent, sums = pl.pallas_call(
        functools.partial(forward_y, cols, slots, width, GMODES),
        grid=(FIELDS,),
        in_specs=state_step
        + state_w
        + [whole(part) for part in wide_y],
        out_specs=[
            pl.BlockSpec((devices, rows_here, 1, cols, lanes), lambda i: (0, 0, i, 0, 0)),
            pl.BlockSpec((2 * groups_here, 8, 128), lambda i: (0, 0, 0)),
        ],
        out_shape=[
            jax.ShapeDtypeStruct((devices, rows_here, FIELDS, cols, lanes), jnp.float32),
            jax.ShapeDtypeStruct((2 * groups_here, 8, 128), jnp.float32),
        ],
        compiler_params=params,
        cost_estimate=pl.CostEstimate(
            flops=2 * 3 * FIELDS * 2 * NY * NY * cols * lanes, bytes_accessed=20 << 20, transcendentals=0
        ),
    )(*[state] * (2 * width), *wide_y)

    group_row = jnp.broadcast_to(kz_group[None, :].astype(jnp.float32), (8, NZ))
    operands = [*wide_z, *x_forward, *x_back, *z_back, group_row, wave_kept, sums]
    final, totals, modes = pl.pallas_call(
        functools.partial(travel, groups, slabs, TWO_PI / NX, GMODES, reach),
        in_specs=[pl.BlockSpec(memory_space=pl.ANY)] + [pl.BlockSpec(memory_space=pltpu.VMEM)] * len(operands),
        out_specs=[pl.BlockSpec(memory_space=pl.ANY)] * 2 + [pl.BlockSpec(memory_space=pltpu.VMEM)],
        out_shape=[
            jax.ShapeDtypeStruct((groups, slabs, rows_here, RETURNS, cols, lanes), jnp.float32),
            jax.ShapeDtypeStruct((slabs, *sums.shape), jnp.float32),
            jax.ShapeDtypeStruct((slots, 128), jnp.float32),
        ],
        scratch_shapes=[
            pltpu.VMEM((2 * NZ, 2 * NZ), jnp.bfloat16),
            pltpu.VMEM((2 * NZ, 2 * NZ), jnp.bfloat16),
            pltpu.VMEM((2 * half, 2 * NZ), jnp.bfloat16),
            pltpu.VMEM((8, 2 * NZ), jnp.float32),
            pltpu.VMEM((rows_here, devices, FIELDS, cols, lanes), jnp.float32),
            pltpu.VMEM((rows_here, slabs, RETURNS, cols, 2 * half), jnp.float32),
            pltpu.VMEM((rows_here, slabs, RETURNS, cols, 2 * half), jnp.float32),
            pltpu.VMEM((rows_here, groups, slabs, RETURNS, cols, lanes), jnp.float32),
        ]
        + [pltpu.SemaphoreType.DMA((rows_here,))] * 3
        + [pltpu.SemaphoreType.DMA((rows_here * len(PARTS),))] * 5
        + [pltpu.SemaphoreType.DMA] * 3,
        compiler_params=pltpu.CompilerParams(vmem_limit_bytes=63 * 1024 * 1024, has_side_effects=True),
    )(sent, *operands)

    block = 8 if cols % 8 == 0 else cols
    return pl.pallas_call(
        functools.partial(finish, slots, width, (NX, NY, NZ), GMODES),
        grid=(cols // block,),
        in_specs=[pl.BlockSpec((groups, slabs, rows_here, RETURNS, block, lanes), lambda i: (0, 0, 0, 0, i, 0))]
        + [pl.BlockSpec((4, 2, slots, block, 128), lambda i, k=k: (0, 0, 0, i, k)) for k in range(width)]
        + [whole(wide_y[0]), whole(wide_y[1]), whole(modes), whole(totals)]
        + [pl.BlockSpec(memory_space=pltpu.SMEM)] * 3,
        out_specs=pl.BlockSpec((4, 2, slots, block, NY), lambda i: (0, 0, 0, i, 0)),
        out_shape=jax.ShapeDtypeStruct(state.shape, jnp.float32),
        scratch_shapes=[pltpu.VMEM((8 * slots * block, 128), jnp.float32)] * width,
        compiler_params=params,
        cost_estimate=pl.CostEstimate(flops=1 << 33, bytes_accessed=28 << 20, transcendentals=0),
    )(final, *[state] * width, *wide_y, modes, totals, cutoffs, damping, power)


def solution(mesh):
    return jax.shard_map(
        shards,
        mesh=mesh,
        in_specs=(P(None, None, "grp", "slab", None), P(), P(), P(), P()),
        out_specs=P(None, None, "grp", "slab", None),
        check_vma=False,
    )
```

```python
import functools
import math

import jax
import jax.numpy as jnp
import numpy as np
from jax import lax
from jax.experimental import pallas as pl
from jax.experimental.pallas import tpu as pltpu
from jax.sharding import PartitionSpec as P

TWO_PI = 6.283185307179586
TIME_STEP = 0.25
CORIOLIS = 1.0
BRUNT_SQUARED = 2.0
EPSILON = 1e-06
AHEAD = 3
LAG = 3
PARTS = ((0, 2), (2, 4), (4, 5))
WIDEST = 32
FIELDS = 6
RETURNS = 5


def signed(index, length):
    return jnp.where(index < length // 2, index, index - length)


def halves(values):
    high = values.astype(jnp.bfloat16)
    low = (values - high.astype(jnp.float32)).astype(jnp.bfloat16)
    return high, low


def constant_halves(table):
    table = np.asarray(table, np.float32)
    high = table.astype(jnp.bfloat16)
    low = (table - high.astype(np.float32)).astype(jnp.bfloat16)
    return jnp.asarray(high), jnp.asarray(low)


def dot3(left, right, dims=(((1,), (0,)), ((), ()))):
    dot = functools.partial(lax.dot_general, dimension_numbers=dims, preferred_element_type=jnp.float32)
    return dot(left[0], right[0]) + (dot(left[0], right[1]) + dot(left[1], right[0]))


def trig(modes, points, length):
    phase = np.asarray(modes)[:, None] * np.asarray(points)[None, :] % length
    theta = phase * (2.0 * math.pi / length)
    return np.cos(theta), np.sin(theta)


def flat_rows(ref):
    shape = ref.shape
    return ref.reshape(math.prod(shape[:-1]), shape[-1])


def strided(ref, start, count, stride):
    return ref[pl.ds(start, count, stride=stride), :]


def forward_y(cols, slots, width, members, *refs):
    flow_w = [flat_rows(ref) for ref in refs[width : 2 * width]]
    high_ref, low_ref, out_ref, sums_ref = refs[2 * width :]
    out = flat_rows(out_ref)
    lanes = 2 * slots
    count = high_ref.shape[0]
    rows = [flat_rows(ref) for ref in refs[:width]]
    table = tuple(jnp.concatenate([ref[:, :count], ref[:, count:]], axis=0) for ref in (high_ref, low_ref))
    mode = signed(lax.broadcasted_iota(jnp.int32, (1, count), 1), count).astype(jnp.float32)
    sloped = (pl.program_id(0) == 1) | (pl.program_id(0) == 3)
    factor = jnp.where(sloped, TWO_PI / count * mode, 1.0)
    sign = jnp.where(lax.broadcasted_iota(jnp.int32, (1, lanes), 1) < slots, -1.0, 1.0)
    pair = 2 if cols % 2 == 0 else 1
    def some(first):
        taken = []
        for j in range(pair):
            for d in range(2):
                start = d * slots * cols + first + j
                taken.append(jnp.concatenate([strided(part, start, slots, cols) for part in rows], axis=1))
        data = halves(jnp.concatenate(taken, axis=0) * factor)
        both = dot3(table, data, (((1,), (1,)), ((), ())))
        for j in range(pair):
            part = both[:, j * lanes : (j + 1) * lanes]
            result = part[:count] + sign * pltpu.roll(part[count:], slots, 1)
            out[pl.ds(first + j, count, stride=cols), :] = result

    for i in range(cols // pair):
        some(i * pair)

    step = pl.program_id(0)
    here = sums_ref.shape[0] // 2
    size = members * cols

    @pl.when(step == 0)
    def _():
        sums_ref[...] = jnp.zeros_like(sums_ref)

    def add_up(which, one, two, weight):
        for group in range(here):
            for d in range(2):
                start = (d * slots + group * members) * cols
                for a, b in zip(one, two):
                    product = a[pl.ds(start, size), :] * b[pl.ds(start, size), :]
                    total = jnp.sum(product.reshape(size // 8, 8, 128), axis=0)
                    sums_ref[which * here + group] += weight * total

    @pl.when((step == 0) | (step == 2) | (step == 4))
    def _():
        add_up(1, rows, rows, 0.5)

    @pl.when(step == 5)
    def _():
        add_up(1, rows, rows, 0.5 / BRUNT_SQUARED)
        add_up(0, rows, flow_w, 1.0)


def planes(groups, slabs, x_step, read, zf_refs, xf_refs, xb_refs, zb_refs, kz_ref, kept_ref, write):
    wave_z = kz_ref[0:1, :]
    nz = zf_refs[0].shape[1] // 2
    u, u_y, w, w_y, v, b = (jnp.concatenate([read(g, f) for g in range(groups)], axis=1) for f in range(FIELDS))
    kx = u.shape[0]
    wave_x = x_step * lax.broadcasted_iota(jnp.int32, (kx, 1), 0).astype(jnp.float32)
    omega_x = w_y - wave_z * v
    omega_y = wave_z * u - wave_x * w
    omega_z = wave_x * v - u_y
    stacked = halves(jnp.concatenate([u, v, w, b, omega_x, omega_y, omega_z], axis=0))
    lines = dot3(stacked, (zf_refs[0][...], zf_refs[1][...]))
    grids = []
    for f in range(7):
        line = lines[f * kx : (f + 1) * kx]
        line = halves(jnp.concatenate([line[:, :nz], line[:, nz:]], axis=0))
        kind = 0 if f < 4 else 1
        grids.append(dot3((xf_refs[0][kind], xf_refs[1][kind]), line))
    gu, gv, gw, gb, gox, goy, goz = grids
    products = [gv * goz - gw * goy, gw * gox - gu * goz, gu * goy - gv * gox, gu * gb, gv * gb, gw * gb]
    table = (xb_refs[0][...], xb_refs[1][...])
    backs = []
    for product in products:
        back = dot3(table, halves(product))
        backs.append(jnp.concatenate([back[:kx], back[kx:]], axis=1))
    spectra = dot3(halves(jnp.concatenate(backs, axis=0)), (zb_refs[0][...], zb_refs[1][...]))
    hats = [spectra[f * kx : (f + 1) * kx] for f in range(6)]
    moved = wave_x * hats[3] + kept_ref[0:1, :] * hats[5]
    for f, hat in enumerate([hats[0], hats[1], hats[2], moved, hats[4]]):
        write(f, hat)


def slot_tables(members, reach, wide, group_ref, g, zf_refs, choose_ref, kz_ref, modes_ref):
    nz = group_ref.shape[1]
    slots = modes_ref.shape[0]
    half = choose_ref.shape[0] // 2
    rows = lax.broadcasted_iota(jnp.int32, (nz, nz), 0)
    lanes = lax.broadcasted_iota(jnp.int32, (nz, nz), 1)
    across = jnp.broadcast_to(group_ref[0:1, :], (nz, nz))
    down = across.T
    same = across == down
    rank_row = jnp.sum(jnp.where(same & (rows < lanes), 1.0, 0.0), axis=0, keepdims=True)
    rank_col = jnp.sum(jnp.where(same & (lanes < rows), 1.0, 0.0), axis=1, keepdims=True)
    place_row = across[0:1, :] * members + rank_row
    place_col = down[:, 0:1] * members + rank_col
    picks = jnp.where(rows.astype(jnp.float32) == place_row, 1.0, 0.0).astype(jnp.bfloat16)
    for part, out in zip(wide, zf_refs):
        chosen = jnp.dot(picks, part[...], preferred_element_type=jnp.float32)
        cosine, sine = chosen[:, :nz], chosen[:, nz:]
        for k in range(nz // slots):
            here = slice(k * slots, (k + 1) * slots)
            start = 2 * k * slots
            out[start : start + slots, :nz] = cosine[here].astype(jnp.bfloat16)
            out[start : start + slots, nz:] = sine[here].astype(jnp.bfloat16)
            out[start + slots : start + 2 * slots, :nz] = (-sine[here]).astype(jnp.bfloat16)
            out[start + slots : start + 2 * slots, nz:] = cosine[here].astype(jnp.bfloat16)
    lane = lax.broadcasted_iota(jnp.int32, (1, 2 * nz), 1)
    slot = (lane // (2 * slots) * slots + lane % slots).astype(jnp.float32)
    mode_col = signed(lax.broadcasted_iota(jnp.int32, (nz, 1), 0), nz).astype(jnp.float32)
    mode = jnp.sum(jnp.where(place_col == slot, mode_col, 0.0), axis=0, keepdims=True)
    kz_ref[...] = jnp.broadcast_to(TWO_PI / nz * mode, kz_ref.shape)
    part = (lane % (2 * slots) >= slots).astype(jnp.int32)
    row = lax.broadcasted_iota(jnp.int32, (half, 1), 0)
    hit = jnp.where((row - reach).astype(jnp.float32) == mode, 1.0, 0.0)
    for d in range(2):
        choose_ref[d * half : (d + 1) * half, :] = jnp.where(part == d, hit, 0.0).astype(jnp.bfloat16)
    mine = (lax.broadcasted_iota(jnp.int32, (slots, 1), 0) + g * slots).astype(jnp.float32)
    mode_row = signed(lax.broadcasted_iota(jnp.int32, (1, nz), 1), nz).astype(jnp.float32)
    own = jnp.sum(jnp.where(place_row == mine, mode_row, 0.0), axis=1, keepdims=True)
    modes_ref[...] = jnp.broadcast_to(own, modes_ref.shape)


def travel(groups, slabs, x_step, members, reach, *refs):
    (sent, wide0, wide1, xf0, xf1, xb0, xb1, zb0, zb1, group_ref, kept_ref, sums_ref, final, totals, modes) = refs[:15]
    zf0, zf1, choose, kz_ref = refs[15:19]
    (taken, made, kept, ready, f_send, f_recv, f_own, b_send, b_recv, c_send, c_recv, c_own, t_send, t_recv, t_own) = refs[19:]
    devices = groups * slabs
    count = taken.shape[0]
    cols, lanes = taken.shape[3:]
    ahead = min(AHEAD, count)
    lag = min(LAG, count)
    g = lax.axis_index("grp")
    s = lax.axis_index("slab")
    me = g * slabs + s

    def remote(source, target, send, recv, to_g, to_s):
        pltpu.make_async_remote_copy(
            src_ref=source,
            dst_ref=target,
            send_sem=send,
            recv_sem=recv,
            device_id={"grp": to_g, "slab": to_s},
            device_id_type=pl.DeviceIdType.MESH,
        ).start()

    def wait_all(ref, sem):
        pltpu.make_async_copy(ref, ref, sem).wait()

    def own_f(y):
        return pltpu.make_async_copy(sent.at[me, y], taken.at[y, me], f_own.at[y])

    def send_f(y):
        own_f(y).start()

        def one(k, carry):
            to = lax.rem(me + k, devices)
            remote(sent.at[to, y], taken.at[y, me], f_send.at[y], f_recv.at[y], to // slabs, lax.rem(to, slabs))
            return carry

        lax.fori_loop(1, devices, one, 0)

    parts = len(PARTS)

    def send_b(y):
        for p, (low, high) in enumerate(PARTS):
            fields = pl.ds(low, high - low)

            def one(k, carry):
                to = lax.rem(s + k, slabs)
                q = y * parts + p
                remote(made.at[y, to, fields], kept.at[y, s, fields], b_send.at[q], b_recv.at[q], g, to)
                return carry

            lax.fori_loop(1, slabs, one, 0)

    def own_c(y, p):
        fields = pl.ds(PARTS[p][0], PARTS[p][1] - PARTS[p][0])
        return pltpu.make_async_copy(ready.at[y, g, :, fields], final.at[g, :, y, fields], c_own.at[y * parts + p])

    def send_c(y, p):
        own_c(y, p).start()
        fields = pl.ds(PARTS[p][0], PARTS[p][1] - PARTS[p][0])
        q = y * parts + p
        for k in range(1, groups):
            to = lax.rem(g + k, groups)
            remote(ready.at[y, to, :, fields], final.at[g, :, y, fields], c_send.at[q], c_recv.at[q], to, s)

    def back(y, p):
        low, high = PARTS[p]
        size = high - low
        wait_all(kept.at[y, pl.ds(0, slabs - 1), pl.ds(low, size)], b_recv.at[y * parts + p])
        data = kept[y, :, low:high]
        upper, lower = halves(data.reshape(slabs * size * cols, data.shape[-1]))
        dot = functools.partial(jnp.dot, preferred_element_type=jnp.float32)
        picked = dot(upper, choose[...]) + dot(lower, choose[...])
        for group in range(groups):
            part = picked[:, group * lanes : (group + 1) * lanes]
            ready[y, group, :, low:high] = part.reshape(slabs, size, cols, lanes)

    own_t = pltpu.make_async_copy(sums_ref, totals.at[s], t_own)

    def first(y, carry):
        send_f(y)
        return carry

    lax.fori_loop(0, ahead, first, 0)
    own_t.start()

    def send_t(k, carry):
        remote(sums_ref, totals.at[s], t_send, t_recv, g, lax.rem(s + k, slabs))
        return carry

    lax.fori_loop(1, slabs, send_t, 0)
    slot_tables(members, reach, (wide0, wide1), group_ref, g, (zf0, zf1), choose, kz_ref, modes)

    def step(t, carry):
        @pl.when(t < count)
        def _():
            own_f(t).wait()
            wait_all(taken.at[t, pl.ds(0, devices - 1)], f_recv.at[t])

            @pl.when(t + ahead < count)
            def _():
                send_f(t + ahead)

            def read(group, f):
                part = taken[t, group * slabs : (group + 1) * slabs, f]
                return part.reshape(slabs * cols, lanes)

            def write(f, value):
                made[t, :, f] = value.reshape(slabs, cols, value.shape[1])

            planes(
                groups, slabs, x_step, read, (zf0, zf1), (xf0, xf1), (xb0, xb1), (zb0, zb1), kz_ref, kept_ref, write
            )
            kept[t, s] = made[t, s]

        @pl.when(t >= lag)
        def _():
            back(t - lag, 0)

        @pl.when(t < count)
        def _():
            send_b(t)

        @pl.when(t >= lag)
        def _():
            send_c(t - lag, 0)
            for p in range(1, parts):
                back(t - lag, p)
                send_c(t - lag, p)

        return carry

    lax.fori_loop(0, count + lag, step, 0)

    def last(y, carry):
        wait_all(taken.at[y, pl.ds(0, devices - 1)], f_send.at[y])
        for p, (low, high) in enumerate(PARTS):
            fields = pl.ds(low, high - low)
            q = y * parts + p
            own_c(y, p).wait()
            wait_all(final.at[pl.ds(0, groups - 1), :, y, fields], c_recv.at[q])
            wait_all(kept.at[y, pl.ds(0, slabs - 1), fields], b_send.at[q])
            wait_all(ready.at[y, pl.ds(0, groups - 1), :, fields], c_send.at[q])
        return carry

    lax.fori_loop(0, count, last, 0)
    own_t.wait()
    wait_all(totals.at[pl.ds(0, slabs - 1)], t_recv)
    wait_all(totals.at[pl.ds(0, slabs - 1)], t_send)


def finish(slots, width, sizes, members, *refs):
    nx, ny, nz = sizes
    state_refs = refs[1 : width + 1]
    high_ref, low_ref, modes_ref, totals_ref, cutoffs_ref, damping_ref, power_ref, out_ref = refs[width + 1 : width + 9]
    out_parts = refs[width + 9 :]
    block = out_ref.shape[3]
    rows = flat_rows(refs[0])
    state = [flat_rows(ref) for ref in state_refs]
    table = (high_ref[...], low_ref[...])
    here = slots // members
    first_group = lax.axis_index("grp") * here
    x_count = pl.num_programs(0) * block
    first_x = lax.axis_index("slab") * x_count + pl.program_id(0) * block
    cells = members * (nx // 2) * ny
    sums = jnp.sum(totals_ref[...], axis=0)
    growths, dampings = [], []
    for group in range(here):
        flux, energy = (
            jnp.sum(jnp.sum(sums[k], axis=0, keepdims=True), axis=1, keepdims=True) / cells
            for k in (group, here + group)
        )
        forcing = (power_ref[first_group + group] - flux) / (2.0 * (energy + EPSILON))
        growths.append(jnp.broadcast_to(1.0 + TIME_STEP * forcing, (members, ny)))
        dampings.append(jnp.full((members, ny), damping_ref[first_group + group], jnp.float32))
    growth = jnp.concatenate(growths, axis=0)
    damping = jnp.concatenate(dampings, axis=0)
    mode_z = jnp.concatenate([modes_ref[...]] * width, axis=1)
    wave_z = TWO_PI / nz * mode_z
    mode_y = signed(lax.broadcasted_iota(jnp.int32, (1, ny), 1), ny).astype(jnp.float32)
    wave_y = TWO_PI / ny * mode_y

    def within(mode, which, length):
        limit = (cutoffs_ref[which] * length).astype(jnp.float32)
        return jnp.where(96.0 * jnp.abs(mode) <= limit, 1.0, 0.0)

    kept_yz = within(mode_z, 2, nz) * within(mode_y, 1, ny) * TIME_STEP

    def load(c, d, x):
        start = (c * 2 + d) * slots * block + x
        return jnp.concatenate([strided(part, start, slots, block) for part in state], axis=1)

    def store(c, d, x, value):
        start = (c * 2 + d) * slots * block + x
        for k in range(width):
            out_parts[k][pl.ds(start, slots, stride=block), :] = value[:, 128 * k : 128 * (k + 1)]

    def one(x):
        columns = [rows[pl.ds(f * block + x, ny, stride=RETURNS * block), :].T for f in range(RETURNS)]
        both = dot3(halves(jnp.concatenate(columns, axis=0)), table)
        tends = []
        for f in range(RETURNS):
            re = both[2 * f * slots : (2 * f + 1) * slots]
            im = both[(2 * f + 1) * slots : (2 * f + 2) * slots]
            tends.append((re[:, :ny] + im[:, ny:], im[:, :ny] - re[:, ny:]))
        mode_x = jnp.full((1, ny), (first_x + x).astype(jnp.float32), jnp.float32)
        wave_x = TWO_PI / nx * mode_x
        kept = kept_yz * within(mode_x, 0, nx)
        wave_sq = wave_x * wave_x + wave_y * wave_y + wave_z * wave_z
        implicit = 1.0 + TIME_STEP * damping * wave_sq
        rotation = TIME_STEP * CORIOLIS
        first = 1.0 / (implicit * implicit + rotation * rotation)
        second = 1.0 / (implicit * implicit + TIME_STEP * TIME_STEP * BRUNT_SQUARED)
        inverse_sq = 1.0 / (wave_sq + (wave_sq == 0).astype(jnp.float32))
        total = [tends[3][d] + wave_y * tends[4][d] for d in range(2)]
        source = [total[1], -total[0]]
        for d in range(2):
            right_x = growth * load(0, d, x) + kept * tends[0][d]
            right_y = growth * load(1, d, x) + kept * tends[1][d]
            right_z = growth * load(2, d, x) + kept * tends[2][d]
            right_b = load(3, d, x) + kept * source[d]
            new_x = (implicit * right_x + rotation * right_y) * first
            new_y = (implicit * right_y - rotation * right_x) * first
            new_z = (implicit * right_z + TIME_STEP * right_b) * second
            new_b = (implicit * right_b - TIME_STEP * BRUNT_SQUARED * right_z) * second
            inner = (wave_x * new_x + wave_y * new_y + wave_z * new_z) * inverse_sq
            store(0, d, x, new_x - wave_x * inner)
            store(1, d, x, new_y - wave_y * inner)
            store(2, d, x, new_z - wave_z * inner)
            store(3, d, x, new_b)

    unrolled = 4 if block % 4 == 0 else 1

    def some(i, carry):
        for k in range(unrolled):
            one(i * unrolled + k)
        return carry

    lax.fori_loop(0, block // unrolled, some, 0)
    for k in range(width):
        for c in range(4):
            for d in range(2):
                size = slots * block
                part = out_parts[k][(c * 2 + d) * size : (c * 2 + d + 1) * size, :]
                out_ref[c, d, :, :, 128 * k : 128 * (k + 1)] = part.reshape(slots, block, 128)


def whole(array):
    return pl.BlockSpec(array.shape, lambda *_: (0,) * array.ndim)


def shards(state, kz_group, cutoffs, damping, power):
    groups = lax.axis_size("grp")
    slabs = lax.axis_size("slab")
    slots = state.shape[2]
    cols = state.shape[3]
    NY = state.shape[4]
    NZ = slots * groups
    KX = cols * slabs
    NX = 2 * KX
    GROUPS = damping.shape[0]
    GMODES = NZ // GROUPS
    devices = groups * slabs
    rows_here = NY // devices
    groups_here = GROUPS // groups
    lanes = 2 * slots
    width = NY // 128
    normalizer = 1.0 / math.sqrt(NX * NY * NZ)

    wide_y = constant_halves(np.concatenate(trig(np.arange(NY), np.arange(NY), NY), axis=1))
    wide_z = wide_y
    if NZ != NY:
        wide_z = constant_halves(np.concatenate(trig(np.arange(NZ), np.arange(NZ), NZ), axis=1))
    reach = WIDEST * NZ // 96
    half = -(-(2 * reach + 1) // 64) * 64
    mode_kept = np.arange(half) - reach
    inside = mode_kept <= reach
    cos_k, sin_k = (part * inside for part in trig(np.arange(NZ), mode_kept, NZ))
    z_back = constant_halves(
        np.concatenate(
            [np.concatenate([cos_k, -sin_k], axis=1), np.concatenate([sin_k, cos_k], axis=1)], axis=0
        )
    )
    wave_kept = np.concatenate([TWO_PI / NZ * mode_kept * inside] * 2)
    wave_kept = jnp.asarray(np.broadcast_to(wave_kept, (8, 2 * half)), jnp.float32)
    cos_x, sin_x = trig(np.arange(NX), np.arange(KX), NX)
    weights = np.where(np.arange(KX) == 0, 1.0, 2.0)[None, :] * normalizer
    x_forward = constant_halves(
        np.stack(
            [
                np.concatenate([cos_x * weights, -sin_x * weights], axis=1),
                np.concatenate([-sin_x * weights, -cos_x * weights], axis=1),
            ]
        )
    )
    x_back = constant_halves(np.concatenate([cos_x.T, -sin_x.T], axis=0) * normalizer)

    params = pltpu.CompilerParams(vmem_limit_bytes=60 * 1024 * 1024)
    state_step = [
        pl.BlockSpec(
            (1, 2, slots, cols, 128),
            lambda i, k=k: (jnp.where(i < 4, i // 2 * 2, (i - 4) * 2 + 1), 0, 0, 0, k),
        )
        for k in range(width)
    ]
    state_w = [pl.BlockSpec((1, 2, slots, cols, 128), lambda i, k=k: (2, 0, 0, 0, k)) for k in range(width)]
    sent, sums = pl.pallas_call(
        functools.partial(forward_y, cols, slots, width, GMODES),
        grid=(FIELDS,),
        in_specs=state_step
        + state_w
        + [whole(part) for part in wide_y],
        out_specs=[
            pl.BlockSpec((devices, rows_here, 1, cols, lanes), lambda i: (0, 0, i, 0, 0)),
            pl.BlockSpec((2 * groups_here, 8, 128), lambda i: (0, 0, 0)),
        ],
        out_shape=[
            jax.ShapeDtypeStruct((devices, rows_here, FIELDS, cols, lanes), jnp.float32),
            jax.ShapeDtypeStruct((2 * groups_here, 8, 128), jnp.float32),
        ],
        compiler_params=params,
        cost_estimate=pl.CostEstimate(
            flops=2 * 3 * FIELDS * 2 * NY * NY * cols * lanes, bytes_accessed=20 << 20, transcendentals=0
        ),
    )(*[state] * (2 * width), *wide_y)

    group_row = jnp.broadcast_to(kz_group[None, :].astype(jnp.float32), (8, NZ))
    operands = [*wide_z, *x_forward, *x_back, *z_back, group_row, wave_kept, sums]
    final, totals, modes = pl.pallas_call(
        functools.partial(travel, groups, slabs, TWO_PI / NX, GMODES, reach),
        in_specs=[pl.BlockSpec(memory_space=pl.ANY)] + [pl.BlockSpec(memory_space=pltpu.VMEM)] * len(operands),
        out_specs=[pl.BlockSpec(memory_space=pl.ANY)] * 2 + [pl.BlockSpec(memory_space=pltpu.VMEM)],
        out_shape=[
            jax.ShapeDtypeStruct((groups, slabs, rows_here, RETURNS, cols, lanes), jnp.float32),
            jax.ShapeDtypeStruct((slabs, *sums.shape), jnp.float32),
            jax.ShapeDtypeStruct((slots, 128), jnp.float32),
        ],
        scratch_shapes=[
            pltpu.VMEM((2 * NZ, 2 * NZ), jnp.bfloat16),
            pltpu.VMEM((2 * NZ, 2 * NZ), jnp.bfloat16),
            pltpu.VMEM((2 * half, 2 * NZ), jnp.bfloat16),
            pltpu.VMEM((8, 2 * NZ), jnp.float32),
            pltpu.VMEM((rows_here, devices, FIELDS, cols, lanes), jnp.float32),
            pltpu.VMEM((rows_here, slabs, RETURNS, cols, 2 * half), jnp.float32),
            pltpu.VMEM((rows_here, slabs, RETURNS, cols, 2 * half), jnp.float32),
            pltpu.VMEM((rows_here, groups, slabs, RETURNS, cols, lanes), jnp.float32),
        ]
        + [pltpu.SemaphoreType.DMA((rows_here,))] * 3
        + [pltpu.SemaphoreType.DMA((rows_here * len(PARTS),))] * 5
        + [pltpu.SemaphoreType.DMA] * 3,
        compiler_params=pltpu.CompilerParams(vmem_limit_bytes=63 * 1024 * 1024, has_side_effects=True),
    )(sent, *operands)

    block = 8 if cols % 8 == 0 else cols
    return pl.pallas_call(
        functools.partial(finish, slots, width, (NX, NY, NZ), GMODES),
        grid=(cols // block,),
        in_specs=[pl.BlockSpec((groups, slabs, rows_here, RETURNS, block, lanes), lambda i: (0, 0, 0, 0, i, 0))]
        + [pl.BlockSpec((4, 2, slots, block, 128), lambda i, k=k: (0, 0, 0, i, k)) for k in range(width)]
        + [whole(wide_y[0]), whole(wide_y[1]), whole(modes), whole(totals)]
        + [pl.BlockSpec(memory_space=pltpu.SMEM)] * 3,
        out_specs=pl.BlockSpec((4, 2, slots, block, NY), lambda i: (0, 0, 0, i, 0)),
        out_shape=jax.ShapeDtypeStruct(state.shape, jnp.float32),
        scratch_shapes=[pltpu.VMEM((8 * slots * block, 128), jnp.float32)] * width,
        compiler_params=params,
        cost_estimate=pl.CostEstimate(flops=1 << 33, bytes_accessed=28 << 20, transcendentals=0),
    )(final, *[state] * width, *wide_y, modes, totals, cutoffs, damping, power)


def solution(mesh):
    return jax.shard_map(
        shards,
        mesh=mesh,
        in_specs=(P(None, None, "grp", "slab", None), P(), P(), P(), P()),
        out_specs=P(None, None, "grp", "slab", None),
        check_vma=False,
    )
```
